32 devices in a mesh: grp: 2 (over y), band: 4 (over z), mem: 2 (over x), fld: 2 (over core).
Axes of the slice: x: 2, y: 2, z: 4, core: 2. Of those that a mesh axis runs over, the one named last changes fastest.
Arguments:
- surface_fields: bfloat16 [16, 8, 8, 65536], P(('grp', 'mem'), 'fld', None, 'band'), parts along dimension 0, may hold values from -8 to 8
- land_mask: int32 [65536], P('band'), may hold values from 0 to 1, as said below
- source_area: float32 [65536], P('band'), may hold values from 0.5 to 1.5
- target_area: float32 [16384], P('band'), may hold values from 0.75 to 1.25
- weight_tiles: bfloat16 [16, 128, 128], replicated, may hold values from -1 to 1
- tile_of: int32 [128, 24], P('band'), may hold values from 0 to 15
- block_of: int32 [128, 24], P('band'), may hold values from 0 to 191, as said below
- live_slots: int32 [128], P('band'), may hold values from 1 to 24, as said below
Outputs:
- regridded: float32 [16, 8, 8, 16384], P(('grp', 'mem'), 'fld', None, 'band'), parts along dimension 0
- conserved: float32 [16, 8, 8], P(('grp', 'mem'), 'fld'), parts along dimension 0
- ensemble: float32 [16, 8], P(('grp', 'fld')), parts along dimension 0
The draws below stay inside these ranges and needn't reach their ends.
There are 2 independent parts, one for each index of `grp`. The reference program is written for one: setup_inputs(seed, part) draws one part's arguments, and reference() takes and returns one part's arrays. A program takes and returns all parts, laid end to end along the dimension named above; an argument that names none is the same for every part. Nothing has to cross between parts.
Inputs may be any that keep to these rules, and one draw needn't show every extreme that they name: `land_mask`: 1 marks ocean, 0 land. `block_of`: for the target block at place j (0 to 31) within its band, every entry lies in 4 * j to 4 * j + 4 + 2 * 32 - 1; values under 32 name the lower band's last blocks, values from 160 on the higher band's first blocks. `live_slots`: slots from this count on are unused.
All inputs are finite; a program needn't handle non-finite values.
Results may differ from the reference program's by a relative error of at most 0.0014.
Values may be sent and summed in bfloat16 or wider, within the bound.
A program may use at most 64 MiB of HBM per device.

```python
import jax
import jax.numpy as jnp
from jax import lax

MEMBERS = 8
FIELDS = 8
SNAPSHOTS = 8
TILE_CELLS = 128
TGT_BLK_DEV = 32
STRIDE = 4
HALO_BLK = 32
SLOT_COUNT = 24
TILE_COUNT = 16
SRC_BLK_DEV = 128
SRC_BLOCKS = 512
TGT_BLOCKS = 128
SRC_CELLS = 65536
TGT_CELLS = 16384


def draw_surface_fields(key, part):
    first_key, second_key, third_key = jax.random.split(key, 3)
    shape = (MEMBERS, FIELDS, SNAPSHOTS, SRC_BLOCKS, TILE_CELLS)
    offset = jax.random.uniform(first_key, (MEMBERS, FIELDS, SNAPSHOTS, 1, 1), jnp.float32, -1.0, 1.0)
    noise = jnp.clip(jax.random.normal(third_key, shape, jnp.float32), -5.0, 5.0)
    regional = 0.5 * jnp.clip(jax.random.normal(second_key, (MEMBERS, FIELDS, SNAPSHOTS, SRC_BLOCKS, 1), jnp.float32), -2.0, 2.0)
    values = offset + regional + noise
    return values.reshape(MEMBERS, FIELDS, SNAPSHOTS, SRC_CELLS).astype(jnp.bfloat16)


def draw_land_mask(key, part):
    first_key, second_key, third_key = jax.random.split(key, 3)
    band_count = SRC_CELLS // (SRC_BLK_DEV * TILE_CELLS)
    band_level = jax.random.randint(first_key, (band_count, 1, 1), 25, 101)
    region_level = jax.random.randint(second_key, (band_count, SRC_BLK_DEV, 1), 40, 101)
    cell_draw = jax.random.randint(third_key, (band_count, SRC_BLK_DEV, TILE_CELLS), 0, 10000)
    ocean = (cell_draw < band_level * region_level).astype(jnp.int32)
    return ocean.reshape(SRC_CELLS)


def draw_weight_tiles(key, part):
    fan = SLOT_COUNT * TILE_CELLS
    shape = (TILE_COUNT, TILE_CELLS, TILE_CELLS)
    noise = jnp.clip(jax.random.normal(key, shape, jnp.float32), -5.0, 5.0)
    mean_part = 1.0
    return ((mean_part + noise * jnp.sqrt(jnp.float32(fan))) / fan).astype(jnp.bfloat16)


def draw_block_of(key, part):
    position = jnp.arange(TGT_BLOCKS, dtype=jnp.int32) % TGT_BLK_DEV
    offsets = jax.random.randint(key, (TGT_BLOCKS, SLOT_COUNT), 0, STRIDE + 2 * HALO_BLK)
    picks = STRIDE * position[:, None] + offsets
    picks = picks.at[0, 0].set(0)
    picks = picks.at[TGT_BLOCKS - 1, 0].set(STRIDE * TGT_BLK_DEV + 2 * HALO_BLK - 1)
    return picks.astype(jnp.int32)


def draw_live_slots(key, part):
    first_key, second_key = jax.random.split(key, 2)
    band_count = TGT_BLOCKS // TGT_BLK_DEV
    tops = jax.random.randint(first_key, (band_count,), SLOT_COUNT // 4 + 1, SLOT_COUNT + 1)
    band_top = jnp.repeat(tops, TGT_BLK_DEV)
    counts = jax.random.randint(second_key, (TGT_BLOCKS,), 1, band_top + 1)
    return counts.at[0].set(SLOT_COUNT).astype(jnp.int32)


def set_ends(array, stream_key, least, largest):
    longest = array.shape.index(max(array.shape))
    spots = []
    for shift in (0, 1):
        where = [jax.random.randint(jax.random.fold_in(stream_key, axis), (), 0, length) for axis, length in enumerate(array.shape)]
        where[longest] = (where[longest] + shift) % array.shape[longest]
        spots.append(tuple(where))
    return array.at[spots[0]].set(least).at[spots[1]].set(largest)


def level_of(key, extent, pieces, least, high):
    factor_of, own = 1.0, jax.random.fold_in(key, 6)
    for dim, blocks in pieces:
        draws = jnp.exp(jax.random.uniform(jax.random.fold_in(own, dim), (blocks,), jnp.float32, least / len(pieces), high / len(pieces)))
        factor_of = factor_of * jnp.repeat(draws, extent[dim] // blocks).reshape([-1 if axis == dim else 1 for axis in range(len(extent))])
    return factor_of


def setup_inputs(seed: int = 0, part: int = 0) -> dict:
    splits = jax.random.split(jax.random.key(seed), 9)
    own_keys = jax.random.split(jax.random.fold_in(splits[8], part), 9)
    return {
        "surface_fields": draw_surface_fields(jax.random.fold_in(jax.random.fold_in(splits[8], part), 71), part),
        "land_mask": draw_land_mask(jax.random.fold_in(splits[8], 71), part),
        "source_area": jnp.clip(0.5 + 1.0 * jax.random.uniform(splits[2], (SRC_CELLS,), jnp.float32) ** level_of(splits[2], (SRC_CELLS,), ((0, 4),), -0.2, 0.2), 0.5, 1.5),
        "target_area": jnp.clip(0.75 + 0.5 * jax.random.uniform(splits[3], (TGT_CELLS,), jnp.float32) ** level_of(splits[3], (TGT_CELLS,), ((0, 4),), -0.2, 0.2), 0.75, 1.25),
        "weight_tiles": draw_weight_tiles(jax.random.fold_in(splits[8], 71), part),
        "tile_of": set_ends(jax.random.randint(splits[5], (TGT_BLOCKS, SLOT_COUNT), 0, TILE_COUNT), jax.random.fold_in(splits[5], 1), 0, TILE_COUNT - 1).astype(jnp.int32),
        "block_of": draw_block_of(jax.random.fold_in(splits[8], 71), part),
        "live_slots": draw_live_slots(jax.random.fold_in(splits[8], 71), part),
    }


def reference(surface_fields, land_mask, source_area, target_area, weight_tiles, tile_of, block_of, live_slots):
    columns = MEMBERS * FIELDS * SNAPSHOTS
    weighted = (source_area * land_mask.astype(jnp.float32) * surface_fields.astype(jnp.float32)).astype(jnp.bfloat16)
    flat = weighted.reshape(columns, SRC_BLOCKS, TILE_CELLS)
    padding = jnp.zeros((columns, HALO_BLK, TILE_CELLS), jnp.bfloat16)
    padded = jnp.concatenate([padding, flat, padding], axis=1)
    owner = jnp.arange(TGT_BLOCKS, dtype=jnp.int32) // TGT_BLK_DEV
    picks = (owner[:, None] * SRC_BLK_DEV + block_of).astype(jnp.int32)

    def one_slot(running, position):
        chosen = jnp.take(padded, picks[:, position], axis=1).astype(jnp.float32)
        weights = jnp.take(weight_tiles, tile_of[:, position], axis=0).astype(jnp.float32)
        usable = (position < live_slots)[:, None, None]
        weights = jnp.where(usable, weights, jnp.zeros((), jnp.float32))
        running = running + jnp.einsum("cnb,nbd->cnd", chosen, weights, precision=lax.Precision.HIGHEST)
        return running, None

    start = jnp.zeros((columns, TGT_BLOCKS, TILE_CELLS), jnp.float32)
    raw_sums, unused = lax.scan(one_slot, start, jnp.arange(SLOT_COUNT, dtype=jnp.int32))
    raw_sums = raw_sums.reshape(columns, TGT_CELLS)
    source_total = jnp.sum(weighted.reshape(columns, SRC_CELLS).astype(jnp.float32), axis=1)
    target_total = jnp.sum(raw_sums, axis=1)
    area_total = jnp.sum(target_area)
    regridded = raw_sums / target_area[None, :] + ((source_total - target_total) / area_total)[:, None]
    conserved = (source_total / area_total).reshape(MEMBERS, FIELDS, SNAPSHOTS)
    ensemble = jnp.sum(conserved, axis=0) / MEMBERS
    return regridded.reshape(MEMBERS, FIELDS, SNAPSHOTS, TGT_CELLS), conserved, ensemble
```

```python
import functools

import jax
import jax.numpy as jnp
from jax import lax
from jax.experimental import pallas as pl
from jax.experimental.pallas import tpu as pltpu
from jax.sharding import PartitionSpec as P

HALO_BLK = 32
SEND_TYPE = jnp.bfloat16
MESH = pl.DeviceIdType.MESH
HBM = pl.BlockSpec(memory_space=pltpu.HBM)
VMEM = pl.BlockSpec(memory_space=pltpu.VMEM)


def row_of(sums):
    return jnp.sum(sums.T, axis=0, keepdims=True)


def slot_dot(source, held, table, n, slots, shift, low, high):
    tiles, blocks, live = table
    used, zero_tile = live(n), held.shape[0] - 1
    left, right = [], []
    for k in range(slots):
        block = blocks(k, n) - shift
        keep = (k < used) & (block >= low) & (block < high)
        left.append(source[jnp.where(keep, block, low)])
        right.append(held[jnp.where(keep, tiles(k, n), zero_tile)])
    return jnp.dot(
        jnp.concatenate(left, axis=1),
        jnp.concatenate(right, axis=0),
        preferred_element_type=jnp.float32,
    )


def main_kernel(
    bands, mems, edge,
    fields, mask_h, area_h, target_area_h, tiles, tile_h, block_h, live_h,
    raw, totals, fix_ref,
    mask, area, target_area, tile_s, block_s, live_s,
    stage, source, held, made, came, rows, landed, target_sum,
    tile_in, block_in, live_in, tile_n, block_n, live_n,
    load_sem, small_sem, list_sem, table_send, table_recv, edge_send, edge_recv, row_send, row_recv,
):
    band, mem = lax.axis_index("band"), lax.axis_index("mem")
    count = bands * mems
    me = mem * bands + band
    own, columns, tile = source.shape
    slots, targets = tile_h.shape
    has_low, has_high = band > 0, band < bands - 1
    chunk = HALO_BLK * tile
    chunks = own // HALO_BLK
    order = [0, chunks - 1] + list(range(1, chunks - 1))

    def place(step):
        other = lax.rem(me + step, count)
        return {"mem": other // bands, "band": lax.rem(other, bands)}

    barrier = pltpu.get_barrier_semaphore()

    def greet(step, carry):
        pl.semaphore_signal(barrier, inc=1, device_id=place(step), device_id_type=MESH)
        return carry

    lax.fori_loop(1, count, greet, 0)

    loads = [
        pltpu.make_async_copy(
            fields.at[:, :, pl.ds(c * chunk, chunk)],
            stage.at[:, :, pl.ds(c * chunk, chunk)],
            load_sem.at[c],
        )
        for c in range(chunks)
    ]
    small = [
        pltpu.make_async_copy(a, b, small_sem.at[i])
        for i, (a, b) in enumerate((
            (mask_h, mask),
            (area_h, area),
            (tiles, held.at[pl.ds(0, tiles.shape[0])]),
            (tile_h, tile_s),
            (block_h, block_s),
            (live_h, live_s),
            (target_area_h, target_area),
        ))
    ]
    small[0].start()
    small[1].start()
    for c in order[:2]:
        loads[c].start()
    for copy in small[2:]:
        copy.start()
    for c in order[2:]:
        loads[c].start()

    pl.semaphore_wait(barrier, count - 1)

    def table_copies(way):
        to = {"band": band - 1 if way == 0 else band + 1}
        pairs = ((tile_h, tile_in), (block_h, block_in), (live_h, live_in))
        return [
            pltpu.make_async_remote_copy(
                src_ref=mine,
                dst_ref=theirs.at[way],
                send_sem=table_send.at[way, i],
                recv_sem=table_recv.at[way, i],
                device_id=to,
                device_id_type=MESH,
            )
            for i, (mine, theirs) in enumerate(pairs)
        ]

    def edge_copy(way, j):
        return pltpu.make_async_remote_copy(
            src_ref=made.at[way, j],
            dst_ref=came.at[way, j],
            send_sem=edge_send.at[way, j],
            recv_sem=edge_recv.at[way, j],
            device_id={"band": band + 1 if way == 0 else band - 1},
            device_id_type=MESH,
        )

    for way, there in ((0, has_low), (1, has_high)):
        @pl.when(there)
        def _(way=way):
            for copy in table_copies(way):
                copy.start()

    held[tiles.shape[0]] = jnp.zeros((tile, tile), held.dtype)

    def fetch(pairs):
        copies = [
            pltpu.make_async_copy(a, b, list_sem.at[i]) for i, (a, b) in enumerate(pairs)
        ]
        for copy in copies:
            copy.start()
        for copy in copies:
            copy.wait()

    def weigh(c, running):
        loads[c].wait()

        def one(n, running):
            at = pl.ds(pl.multiple_of(n * tile, tile), tile)
            scale = area[:, at] * mask[:, at].astype(jnp.float32)
            part = stage[:, :, at].astype(jnp.float32).reshape(columns, tile) * scale
            part = part.astype(source.dtype)
            source[n] = part
            return running + part.astype(jnp.float32)

        return lax.fori_loop(c * HALO_BLK, (c + 1) * HALO_BLK, one, running, unroll=4)

    source_sum = jnp.zeros((columns, tile), jnp.float32)
    small[0].wait()
    small[1].wait()
    for c in order:
        source_sum = weigh(c, source_sum)

    own_table = (
        lambda k, n: tile_s[k, n],
        lambda k, n: block_s[k, n],
        lambda n: live_s[0, n],
    )

    def own_group(first, width, carry):
        for u in range(width):
            t = first + u
            at = pl.ds(pl.multiple_of(t * tile, tile), tile)
            value = slot_dot(source, held, own_table, t, slots, HALO_BLK, 0, own)
            raw[t] = value * (1.0 / target_area[:, at])
            carry = carry + value
        return carry

    for copy in small[2:]:
        copy.wait()
    target_sum[...] = own_group(0, edge // 2, jnp.zeros((columns, tile), jnp.float32))

    for way, there in ((0, has_high), (1, has_low)):
        @pl.when(there)
        def _(way=way):
            for copy in table_copies(way):
                copy.wait_recv()
            pairs = ((tile_in, tile_n), (block_in, block_n), (live_in, live_n))
            fetch([(a.at[way], b.at[way]) for a, b in pairs])

        @pl.when(jnp.logical_not(there))
        def _(way=way):
            pairs = ((tile_h, tile_n), (block_h, block_n), (live_h, live_n))
            fetch([(a, b.at[way]) for a, b in pairs])

    reaches = (
        (HALO_BLK - own, own - HALO_BLK, own),
        (HALO_BLK + own, 0, HALO_BLK),
    )

    def one_edge(j, carry):
        for way, there in ((0, has_high), (1, has_low)):
            table = (
                lambda k, n, way=way: tile_n[way, k, n],
                lambda k, n, way=way: block_n[way, k, n],
                lambda n, way=way: live_n[way, 0, n],
            )
            first = 0 if way == 0 else targets - edge
            value = slot_dot(source, held, table, first + j, slots, *reaches[way])
            made[way, j] = value.astype(made.dtype)
            carry = carry + value * there.astype(jnp.float32)

        for way, there in ((0, has_high), (1, has_low)):
            @pl.when((j > 0) & there)
            def _(way=way):
                edge_copy(way, j - 1).start()

        return carry

    edge_total = lax.fori_loop(0, edge, one_edge, target_sum[...])
    target_sum[...] = edge_total

    target_sum[...] = own_group(edge // 2, edge // 2, target_sum[...])
    for way, there in ((0, has_high), (1, has_low)):
        @pl.when(there)
        def _(way=way):
            edge_copy(way, edge - 1).start()

    target_total = lax.fori_loop(
        1, targets // edge, lambda g, carry: own_group(g * edge, edge, carry), target_sum[...]
    )
    rows[0:1, :] = row_of(source_sum)
    rows[1:2, :] = row_of(target_total)
    rows[2:3, :] = jnp.broadcast_to(
        jnp.sum(target_area[...], axis=1, keepdims=True), (1, columns)
    )
    rows[3:8, :] = jnp.zeros((5, columns), jnp.float32)

    def row_copy(step):
        return pltpu.make_async_remote_copy(
            src_ref=rows,
            dst_ref=landed.at[step],
            send_sem=row_send.at[step],
            recv_sem=row_recv.at[step],
            device_id=place(step),
            device_id_type=MESH,
        )

    def begin(step, carry):
        row_copy(step).start()
        return carry

    def end(step, carry):
        row_copy(step).wait()
        return carry

    for way, there in ((0, has_low), (1, has_high)):
        @pl.when(there)
        def _(way=way):
            for copy in table_copies(way):
                copy.wait_send()

    lax.fori_loop(1, count, begin, 0)
    landed[0] = rows[...]

    for way, there in ((0, has_low), (1, has_high)):
        @pl.when(there)
        def _(way=way):
            def add(j, carry):
                edge_copy(way, j).wait_recv()
                t = j if way == 0 else targets - edge + j
                at = pl.ds(pl.multiple_of(t * tile, tile), tile)
                share = 1.0 / target_area[:, at]
                raw[t] = raw[t] + came[way, j].astype(jnp.float32) * share
                return carry

            lax.fori_loop(0, edge, add, 0)

    for way, there in ((0, has_high), (1, has_low)):
        @pl.when(there)
        def _(way=way):
            def sent(j, carry):
                edge_copy(way, j).wait_send()
                return carry

            lax.fori_loop(0, edge, sent, 0)

    lax.fori_loop(1, count, end, 0)
    for m in range(mems):
        total = jnp.zeros(rows.shape, jnp.float32)
        for b in range(bands):
            total = total + landed[lax.rem(me - (m * bands + b) + count, count)]
        totals[m] = total
    mine = totals[mem]
    fix = (mine[0:1, :] - mine[1:2, :]) / mine[2:3, :]
    fix_ref[...] = jnp.broadcast_to(fix, (fix_ref.shape[1], fix.shape[1])).T


def main_call(fields, mask, area, target_area, tiles, tile_t, block_t, live):
    bands, mems = lax.axis_size("band"), lax.axis_size("mem")
    rows, snaps, cells = fields.shape
    columns = rows * snaps
    slots, targets = tile_t.shape
    count, tile = tiles.shape[0], tiles.shape[1]
    own = cells // tile
    edge = HALO_BLK // (own // targets)
    dma = pltpu.SemaphoreType.DMA
    peers = bands * mems
    return pl.pallas_call(
        functools.partial(main_kernel, bands, mems, edge),
        in_specs=[HBM] * 8,
        out_specs=(VMEM, VMEM, VMEM),
        out_shape=(
            jax.ShapeDtypeStruct((targets, columns, tile), jnp.float32),
            jax.ShapeDtypeStruct((mems, 8, columns), jnp.float32),
            jax.ShapeDtypeStruct((columns, tile), jnp.float32),
        ),
        scratch_shapes=[
            pltpu.VMEM(mask.shape, mask.dtype),
            pltpu.VMEM(area.shape, area.dtype),
            pltpu.VMEM(target_area.shape, target_area.dtype),
            pltpu.SMEM(tile_t.shape, tile_t.dtype),
            pltpu.SMEM(block_t.shape, block_t.dtype),
            pltpu.SMEM(live.shape, live.dtype),
            pltpu.VMEM(fields.shape, fields.dtype),
            pltpu.VMEM((own, columns, tile), jnp.bfloat16),
            pltpu.VMEM((count + 1, tile, tile), tiles.dtype),
            pltpu.VMEM((2, edge, columns, tile), SEND_TYPE),
            pltpu.VMEM((2, edge, columns, tile), SEND_TYPE),
            pltpu.VMEM((8, columns), jnp.float32),
            pltpu.VMEM((peers, 8, columns), jnp.float32),
            pltpu.VMEM((columns, tile), jnp.float32),
            pltpu.VMEM((2, slots, targets), jnp.int32),
            pltpu.VMEM((2, slots, targets), jnp.int32),
            pltpu.VMEM((2, 1, targets), jnp.int32),
            pltpu.SMEM((2, slots, targets), jnp.int32),
            pltpu.SMEM((2, slots, targets), jnp.int32),
            pltpu.SMEM((2, 1, targets), jnp.int32),
            dma((own // HALO_BLK,)),
            dma((7,)),
            dma((3,)),
            dma((2, 3)),
            dma((2, 3)),
            dma((2, edge)),
            dma((2, edge)),
            dma((peers,)),
            dma((peers,)),
        ],
        compiler_params=pltpu.CompilerParams(
            collective_id=0, has_side_effects=True, vmem_limit_bytes=32 << 20
        ),
    )(*[pltpu.with_memory_space_constraint(a, pltpu.HBM) for a in (fields, mask, area, target_area, tiles, tile_t, block_t, live)])


def finish_kernel(fields, snaps, raw_ref, fix_ref, totals_ref, out_ref, mean_ref, ensemble_ref):
    count, columns, tile = raw_ref.shape
    fix = fix_ref[...]
    for n in range(count):
        value = raw_ref[n] + fix
        out_ref[:, :, n * tile:(n + 1) * tile] = value.reshape(columns // snaps, snaps, tile)

    @pl.when(pl.program_id(0) == 1)
    def _():
        mems, members = totals_ref.shape[0], mean_ref.shape[0]
        spot = lax.broadcasted_iota(jnp.int32, (columns, tile), 0)
        lane = lax.broadcasted_iota(jnp.int32, (columns, tile), 1)
        chosen = lax.rem(spot, snaps) == lane
        summed = jnp.zeros((fields, snaps), jnp.float32)

        def table(m):
            row = totals_ref[m, 0:1, :] / totals_ref[m, 2:3, :]
            column = jnp.broadcast_to(row, (tile, columns)).T
            spread = jnp.where(chosen, column, 0.0).reshape(columns // snaps, snaps, tile)
            return jnp.sum(spread, axis=1)[:, 0:snaps]

        mine = table(lax.axis_index("mem"))
        for n in range(members):
            mean_ref[n] = mine[n * fields:(n + 1) * fields]
        for m in range(mems):
            all_of = table(m)
            for n in range(members):
                summed = summed + all_of[n * fields:(n + 1) * fields]
        ensemble_ref[...] = summed / (mems * members)


def finish(raw, fix, totals, members, fields, snaps):
    targets, columns, tile = raw.shape
    steps = 2
    part = targets // steps
    rows = members * fields
    return pl.pallas_call(
        functools.partial(finish_kernel, fields, snaps),
        grid=(steps,),
        in_specs=[
            pl.BlockSpec((part, columns, tile), lambda i: (i, 0, 0)),
            pl.BlockSpec((columns, tile), lambda i: (0, 0)),
            pl.BlockSpec(totals.shape, lambda i: (0, 0, 0)),
        ],
        out_specs=(
            pl.BlockSpec((rows, snaps, part * tile), lambda i: (0, 0, i)),
            pl.BlockSpec((members, fields, snaps), lambda i: (0, 0, 0)),
            pl.BlockSpec((fields, snaps), lambda i: (0, 0)),
        ),
        out_shape=(
            jax.ShapeDtypeStruct((rows, snaps, targets * tile), jnp.float32),
            jax.ShapeDtypeStruct((members, fields, snaps), jnp.float32),
            jax.ShapeDtypeStruct((fields, snaps), jnp.float32),
        ),
        compiler_params=pltpu.CompilerParams(vmem_limit_bytes=16 << 20),
    )(raw, fix, totals)


def on_device(
    surface_fields, land_mask, source_area, target_area, weight_tiles, tile_of, block_of, live_slots
):
    members, fields, snaps, cells = surface_fields.shape
    targets = tile_of.shape[0]
    target_cells = target_area.shape[0]
    raw, totals, fix = main_call(
        surface_fields.reshape(members * fields, snaps, cells),
        land_mask.reshape(1, cells),
        source_area.reshape(1, cells),
        target_area.reshape(1, target_cells),
        weight_tiles,
        tile_of.T,
        block_of.T,
        live_slots.reshape(1, targets),
    )
    regridded, conserved, ensemble = finish(raw, fix, totals, members, fields, snaps)
    return regridded.reshape(members, fields, snaps, target_cells), conserved, ensemble


def solution(mesh):
    placed = (
        P(("grp", "mem"), "fld", None, "band"),
        P("band"),
        P("band"),
        P("band"),
        P(),
        P("band", None),
        P("band", None),
        P("band"),
    )
    return jax.shard_map(
        on_device,
        mesh=mesh,
        in_specs=placed,
        out_specs=(
            P(("grp", "mem"), "fld", None, "band"),
            P(("grp", "mem"), "fld", None),
            P(("grp", "fld"), None),
        ),
        check_vma=False,
    )
```

```python
import functools

import jax
import jax.numpy as jnp
from jax import lax
from jax.experimental import pallas as pl
from jax.experimental.pallas import tpu as pltpu
from jax.sharding import PartitionSpec as P

HALO_BLK = 32
SEND_TYPE = jnp.bfloat16
MESH = pl.DeviceIdType.MESH
HBM = pl.BlockSpec(memory_space=pltpu.HBM)
VMEM = pl.BlockSpec(memory_space=pltpu.VMEM)


def row_of(sums):
    return jnp.sum(sums.T, axis=0, keepdims=True)


def slot_dot(source, held, table, n, slots, shift, low, high):
    used, zero_tile = table[2 * slots, n], held.shape[0] - 1
    left, right = [], []
    for k in range(slots):
        block = table[slots + k, n] - shift
        keep = (k < used) & (block >= low) & (block < high)
        left.append(source[jnp.where(keep, block, low)])
        right.append(held[jnp.where(keep, table[k, n], zero_tile)])
    return jnp.dot(
        jnp.concatenate(left, axis=1),
        jnp.concatenate(right, axis=0),
        preferred_element_type=jnp.float32,
    )


def slot_marks(table, slots, shift, there, own, count):
    targets = table.shape[1]
    pieces = slots // 8
    blank = jnp.full((8, 128 - pieces * targets), -1, jnp.int32)
    live = (lax.broadcasted_iota(jnp.int32, (slots, targets), 0) < table[2 * slots:2 * slots + 1]) & there
    blocks = jnp.where(live, table[slots:2 * slots] - shift, -1)
    kinds = table[0:slots]
    rows = [jnp.concatenate([a[8 * p:8 * p + 8] for p in range(pieces)] + [blank], axis=1) for a in (blocks, kinds)]
    spot = lax.broadcasted_iota(jnp.int32, (own, 128), 0)
    kind = lax.broadcasted_iota(jnp.int32, (count, 128), 0)
    left = [jnp.where(rows[0][r:r + 1] == spot, 1.0, 0.0).astype(jnp.bfloat16) for r in range(8)]
    right = [jnp.where(rows[1][r:r + 1] == kind, 1.0, 0.0).astype(jnp.bfloat16) for r in range(8)]
    return left, right


def main_kernel(
    bands, mems, edge,
    fields, mask_h, area_h, target_area_h, tiles, tile_h, block_h, live_h,
    raw, totals, fix_ref,
    mask, area, target_area, table_v, table_s, near_v, near_s,
    stage, source, held, made, came, rows, landed, source_sum, target_sum, tile_sum, coef,
    load_sem, small_sem, near_sem, table_send, table_recv, edge_send, edge_recv, row_send, row_recv, token,
):
    band, mem = lax.axis_index("band"), lax.axis_index("mem")
    count = bands * mems
    me = mem * bands + band
    own, columns, tile = source.shape
    slots, targets = tile_h.shape
    kinds = tiles.shape[0]
    has_low, has_high = band > 0, band < bands - 1
    chunk = HALO_BLK * tile
    chunks = own // HALO_BLK
    order = [0, chunks - 1] + list(range(1, chunks - 1))
    ways = ((0, has_high), (1, has_low))

    def neighbour(way):
        return {"band": band + 1 if way == 0 else band - 1}

    barrier = pltpu.get_barrier_semaphore()
    for way, there in ways:
        @pl.when(there)
        def _(way=way):
            pl.semaphore_signal(barrier, inc=1, device_id=neighbour(way), device_id_type=MESH)
    for step in range(1, mems):
        pl.semaphore_signal(
            barrier, inc=1, device_id={"mem": lax.rem(mem + step, mems)}, device_id_type=MESH
        )

    loads = [
        pltpu.make_async_copy(
            fields.at[:, :, pl.ds(c * chunk, chunk)],
            stage.at[:, :, pl.ds(c * chunk, chunk)],
            load_sem.at[c],
        )
        for c in range(chunks)
    ]
    lists = ((tile_h, pl.ds(0, slots)), (block_h, pl.ds(slots, slots)), (live_h, pl.ds(2 * slots, 1)))
    small = [
        pltpu.make_async_copy(a, b, small_sem.at[i])
        for i, (a, b) in enumerate(
            [(a, table_v.at[at]) for a, at in lists]
            + [(mask_h, mask), (area_h, area)]
            + [(a, table_s.at[at]) for a, at in lists]
            + [(tiles, held.at[pl.ds(0, kinds)]), (target_area_h, target_area)]
        )
    ]
    for copy in small[:5]:
        copy.start()
    for c in order[:2]:
        loads[c].start()
    for copy in small[5:]:
        copy.start()
    for c in order[2:]:
        loads[c].start()

    def stand_in(way):
        return [
            pltpu.make_async_copy(a, b.at[way, at], near_sem.at[way, i])
            for i, (a, b, at) in enumerate(
                [(a, near_v, at) for a, at in lists] + [(a, near_s, at) for a, at in lists]
            )
        ]

    for way, there in ways:
        @pl.when(jnp.logical_not(there))
        def _(way=way):
            for copy in stand_in(way):
                copy.start()

    def table_copies(way):
        return [
            pltpu.make_async_remote_copy(
                src_ref=table_v,
                dst_ref=theirs.at[1 - way],
                send_sem=table_send.at[way, i],
                recv_sem=table_recv.at[1 - way, i],
                device_id=neighbour(way),
                device_id_type=MESH,
            )
            for i, theirs in enumerate((near_s, near_v))
        ]

    def edge_copy(way, j):
        return pltpu.make_async_remote_copy(
            src_ref=made.at[way, j],
            dst_ref=came.at[way, j],
            send_sem=edge_send.at[way, j],
            recv_sem=edge_recv.at[way, j],
            device_id=neighbour(way),
            device_id_type=MESH,
        )

    held[kinds] = jnp.zeros((tile, tile), held.dtype)
    source_sum[...] = jnp.zeros((columns, tile), jnp.float32)
    target_sum[...] = jnp.zeros((columns, tile), jnp.float32)

    def weigh(c):
        loads[c].wait()

        def one(n, running):
            at = pl.ds(pl.multiple_of(n * tile, tile), tile)
            scale = area[:, at] * mask[:, at].astype(jnp.float32)
            part = stage[:, :, at].astype(jnp.float32).reshape(columns, tile) * scale
            part = part.astype(source.dtype)
            source[n] = part
            return running + part.astype(jnp.float32)

        source_sum[...] = lax.fori_loop(
            c * HALO_BLK, (c + 1) * HALO_BLK, one, source_sum[...], unroll=4
        )

    def token_step(up, down):
        for way, at, first in ((0, up, band == 0), (1, down, band == bands - 1)):
            there = has_high if way == 0 else has_low

            @pl.when(at & jnp.logical_not(first))
            def _(way=way):
                pl.semaphore_wait(token.at[way], 1)

            @pl.when(at & there)
            def _(way=way):
                pl.semaphore_signal(
                    token.at[way], inc=1, device_id=neighbour(way), device_id_type=MESH
                )

    for copy in small[3:5]:
        copy.wait()
    weigh(order[0])
    for copy in small[:3]:
        copy.wait()
    pl.semaphore_wait(
        barrier, has_low.astype(jnp.int32) + has_high.astype(jnp.int32) + (mems - 1)
    )
    for way, there in ways:
        @pl.when(there)
        def _(way=way):
            for copy in table_copies(way):
                copy.start()
    token_step(band == 0, band == bands - 1)
    for c in order[1:]:
        weigh(c)
    token_step(band == 1, band == bands - 2)

    def own_dot(t):
        at = pl.ds(pl.multiple_of(t * tile, tile), tile)
        value = slot_dot(source, held, table_s, t, slots, HALO_BLK, 0, own)
        raw[t] = value * (1.0 / target_area[:, at])

    for copy in small[5:]:
        copy.wait()
    sums = lax.dot_general(
        jnp.ones((16, tile), held.dtype),
        held[pl.ds(0, kinds)].reshape(kinds * tile, tile),
        (((1,), (1,)), ((), ())),
        preferred_element_type=jnp.float32,
    )
    for m in range(kinds):
        tile_sum[m:m + 1, :] = sums[0:1, m * tile:(m + 1) * tile]
    for t in range(edge // 2):
        own_dot(t)

    for way, there in ways:
        @pl.when(there)
        def _(way=way):
            for copy in table_copies(1 - way):
                copy.wait_recv()

        @pl.when(jnp.logical_not(there))
        def _(way=way):
            for copy in stand_in(way):
                copy.wait()

    token_step(band == 2, band == bands - 3)

    reaches = (
        (HALO_BLK - own, own - HALO_BLK, own),
        (HALO_BLK + own, 0, HALO_BLK),
    )
    left, right = slot_marks(table_v[...], slots, HALO_BLK, True, own, kinds)
    for way, there in ways:
        a, b = slot_marks(near_v[way], slots, reaches[way][0], there, own, kinds)
        left, right = left + a, right + b
    uses = lax.dot_general(
        jnp.concatenate(left, axis=1),
        jnp.concatenate(right, axis=1),
        (((1,), (1,)), ((), ())),
        preferred_element_type=jnp.float32,
    )
    coef[...] = jnp.dot(
        uses, tile_sum[...], precision=lax.Precision.HIGHEST, preferred_element_type=jnp.float32
    )

    per = own // edge

    def one_edge(j, carry):
        for way, there in ways:
            first = 0 if way == 0 else targets - edge
            value = slot_dot(source, held, near_s.at[way], first + j, slots, *reaches[way])
            made[way, j] = value.astype(made.dtype)
        own_dot(edge // 2 + j)
        total = target_sum[...]
        for i in range(per):
            s = j * per + i
            total = total + source[s].astype(jnp.float32) * coef[pl.ds(s, 1), :]
        target_sum[...] = total
        for way, there in ways:
            @pl.when(there)
            def _(way=way):
                edge_copy(way, j).start()
        return carry

    lax.fori_loop(0, edge, one_edge, 0)

    rows[0:1, :] = row_of(source_sum[...])
    rows[1:2, :] = row_of(target_sum[...])
    rows[2:3, :] = jnp.broadcast_to(
        jnp.sum(target_area[...], axis=1, keepdims=True), (1, columns)
    )
    rows[3:8, :] = jnp.zeros((5, columns), jnp.float32)

    def place(step):
        other = lax.rem(me + step, count)
        return {"mem": other // bands, "band": lax.rem(other, bands)}

    def row_copy(step):
        return pltpu.make_async_remote_copy(
            src_ref=rows,
            dst_ref=landed.at[step],
            send_sem=row_send.at[step],
            recv_sem=row_recv.at[step],
            device_id=place(step),
            device_id_type=MESH,
        )

    def begin(step, carry):
        row_copy(step).start()
        return carry

    def end(step, carry):
        row_copy(step).wait()
        return carry

    token_step(band > 2, band < bands - 3)
    lax.fori_loop(1, count, begin, 0)
    landed[0] = rows[...]

    done = edge // 2 + edge
    for t in range(done, 2 * edge):
        own_dot(t)

    def own_group(g, carry):
        for u in range(edge):
            own_dot(g * edge + u)
        return carry

    lax.fori_loop(2, targets // edge, own_group, 0)

    for way, there in ways:
        @pl.when(there)
        def _(way=way):
            for copy in table_copies(way):
                copy.wait_send()

    lax.fori_loop(1, count, end, 0)
    for m in range(mems):
        total = jnp.zeros(rows.shape, jnp.float32)
        for b in range(bands):
            total = total + landed[lax.rem(me - (m * bands + b) + count, count)]
        totals[m] = total
    mine = totals[mem]
    fix = (mine[0:1, :] - mine[1:2, :]) / mine[2:3, :]
    fix_ref[...] = jnp.broadcast_to(fix, (fix_ref.shape[1], fix.shape[1])).T

    def add(j, carry):
        for way, there in ((0, has_low), (1, has_high)):
            @pl.when(there)
            def _(way=way):
                edge_copy(way, j).wait_recv()
                t = j if way == 0 else targets - edge + j
                at = pl.ds(pl.multiple_of(t * tile, tile), tile)
                share = 1.0 / target_area[:, at]
                raw[t] = raw[t] + came[way, j].astype(jnp.float32) * share
        return carry

    lax.fori_loop(0, edge, add, 0)

    for way, there in ways:
        @pl.when(there)
        def _(way=way):
            def sent(j, carry):
                edge_copy(way, j).wait_send()
                return carry

            lax.fori_loop(0, edge, sent, 0)


def main_call(fields, mask, area, target_area, tiles, tile_t, block_t, live):
    bands, mems = lax.axis_size("band"), lax.axis_size("mem")
    rows, snaps, cells = fields.shape
    columns = rows * snaps
    slots, targets = tile_t.shape
    count, tile = tiles.shape[0], tiles.shape[1]
    own = cells // tile
    edge = HALO_BLK // (own // targets)
    dma = pltpu.SemaphoreType.DMA
    peers = bands * mems
    lines = 2 * slots + 1
    return pl.pallas_call(
        functools.partial(main_kernel, bands, mems, edge),
        in_specs=[HBM] * 8,
        out_specs=(VMEM, VMEM, VMEM),
        out_shape=(
            jax.ShapeDtypeStruct((targets, columns, tile), jnp.float32),
            jax.ShapeDtypeStruct((mems, 8, columns), jnp.float32),
            jax.ShapeDtypeStruct((columns, tile), jnp.float32),
        ),
        scratch_shapes=[
            pltpu.VMEM(mask.shape, mask.dtype),
            pltpu.VMEM(area.shape, area.dtype),
            pltpu.VMEM(target_area.shape, target_area.dtype),
            pltpu.VMEM((lines, targets), jnp.int32),
            pltpu.SMEM((lines, targets), jnp.int32),
            pltpu.VMEM((2, lines, targets), jnp.int32),
            pltpu.SMEM((2, lines, targets), jnp.int32),
            pltpu.VMEM(fields.shape, fields.dtype),
            pltpu.VMEM((own, columns, tile), jnp.bfloat16),
            pltpu.VMEM((count + 1, tile, tile), tiles.dtype),
            pltpu.VMEM((2, edge, columns, tile), SEND_TYPE),
            pltpu.VMEM((2, edge, columns, tile), SEND_TYPE),
            pltpu.VMEM((8, columns), jnp.float32),
            pltpu.VMEM((peers, 8, columns), jnp.float32),
            pltpu.VMEM((columns, tile), jnp.float32),
            pltpu.VMEM((columns, tile), jnp.float32),
            pltpu.VMEM((count, tile), jnp.float32),
            pltpu.VMEM((own, tile), jnp.float32),
            dma((own // HALO_BLK,)),
            dma((10,)),
            dma((2, 6)),
            dma((2, 2)),
            dma((2, 2)),
            dma((2, edge)),
            dma((2, edge)),
            dma((peers,)),
            dma((peers,)),
            pltpu.SemaphoreType.REGULAR((2,)),
        ],
        compiler_params=pltpu.CompilerParams(
            collective_id=0, has_side_effects=True, vmem_limit_bytes=32 << 20
        ),
    )(*[pltpu.with_memory_space_constraint(a, pltpu.HBM) for a in (fields, mask, area, target_area, tiles, tile_t, block_t, live)])


def finish_kernel(fields, snaps, raw_ref, fix_ref, totals_ref, out_ref, mean_ref, ensemble_ref):
    count, columns, tile = raw_ref.shape
    fix = fix_ref[...]
    for n in range(count):
        value = raw_ref[n] + fix
        out_ref[:, :, n * tile:(n + 1) * tile] = value.reshape(columns // snaps, snaps, tile)

    @pl.when(pl.program_id(0) == 1)
    def _():
        mems, members = totals_ref.shape[0], mean_ref.shape[0]
        spot = lax.broadcasted_iota(jnp.int32, (columns, tile), 0)
        lane = lax.broadcasted_iota(jnp.int32, (columns, tile), 1)
        chosen = lax.rem(spot, snaps) == lane
        summed = jnp.zeros((fields, snaps), jnp.float32)

        def table(m):
            row = totals_ref[m, 0:1, :] / totals_ref[m, 2:3, :]
            column = jnp.broadcast_to(row, (tile, columns)).T
            spread = jnp.where(chosen, column, 0.0).reshape(columns // snaps, snaps, tile)
            return jnp.sum(spread, axis=1)[:, 0:snaps]

        mine = table(lax.axis_index("mem"))
        for n in range(members):
            mean_ref[n] = mine[n * fields:(n + 1) * fields]
        for m in range(mems):
            all_of = table(m)
            for n in range(members):
                summed = summed + all_of[n * fields:(n + 1) * fields]
        ensemble_ref[...] = summed / (mems * members)


def finish(raw, fix, totals, members, fields, snaps):
    targets, columns, tile = raw.shape
    steps = 2
    part = targets // steps
    rows = members * fields
    return pl.pallas_call(
        functools.partial(finish_kernel, fields, snaps),
        grid=(steps,),
        in_specs=[
            pl.BlockSpec((part, columns, tile), lambda i: (i, 0, 0)),
            pl.BlockSpec((columns, tile), lambda i: (0, 0)),
            pl.BlockSpec(totals.shape, lambda i: (0, 0, 0)),
        ],
        out_specs=(
            pl.BlockSpec((rows, snaps, part * tile), lambda i: (0, 0, i)),
            pl.BlockSpec((members, fields, snaps), lambda i: (0, 0, 0)),
            pl.BlockSpec((fields, snaps), lambda i: (0, 0)),
        ),
        out_shape=(
            jax.ShapeDtypeStruct((rows, snaps, targets * tile), jnp.float32),
            jax.ShapeDtypeStruct((members, fields, snaps), jnp.float32),
            jax.ShapeDtypeStruct((fields, snaps), jnp.float32),
        ),
        compiler_params=pltpu.CompilerParams(vmem_limit_bytes=16 << 20),
    )(raw, fix, totals)


def on_device(
    surface_fields, land_mask, source_area, target_area, weight_tiles, tile_of, block_of, live_slots
):
    members, fields, snaps, cells = surface_fields.shape
    targets = tile_of.shape[0]
    target_cells = target_area.shape[0]
    raw, totals, fix = main_call(
        surface_fields.reshape(members * fields, snaps, cells),
        land_mask.reshape(1, cells),
        source_area.reshape(1, cells),
        target_area.reshape(1, target_cells),
        weight_tiles,
        tile_of.T,
        block_of.T,
        live_slots.reshape(1, targets),
    )
    regridded, conserved, ensemble = finish(raw, fix, totals, members, fields, snaps)
    return regridded.reshape(members, fields, snaps, target_cells), conserved, ensemble


def solution(mesh):
    placed = (
        P(("grp", "mem"), "fld", None, "band"),
        P("band"),
        P("band"),
        P("band"),
        P(),
        P("band", None),
        P("band", None),
        P("band"),
    )
    return jax.shard_map(
        on_device,
        mesh=mesh,
        in_specs=placed,
        out_specs=(
            P(("grp", "mem"), "fld", None, "band"),
            P(("grp", "mem"), "fld", None),
            P(("grp", "fld"), None),
        ),
        check_vma=False,
    )
```

```python
import functools

import jax
import jax.numpy as jnp
from jax import lax
from jax.experimental import pallas as pl
from jax.experimental.pallas import tpu as pltpu
from jax.sharding import PartitionSpec as P

HALO_BLK = 32
RING = 3
EARLY = 12
SEND_TYPE = jnp.bfloat16
MESH = pl.DeviceIdType.MESH
HBM = pl.BlockSpec(memory_space=pltpu.HBM)
VMEM = pl.BlockSpec(memory_space=pltpu.VMEM)


def row_of(sums):
    return jnp.sum(sums.T, axis=0, keepdims=True)


def slot_pair(source, held, job, p):
    table, n, slots, shift, low, high = job
    tile, zero_tile = held.shape[1], held.shape[0] - 1
    left, right = [], []
    for k in (2 * p, 2 * p + 1):
        block = table[slots + k, n] - shift
        keep = (k < table[2 * slots, n]) & (block >= low) & (block < high)
        left.append(source[jnp.where(keep, block, low)])
        right.append(held[jnp.where(keep, table[k, n], zero_tile)])
    right = jnp.concatenate(right, axis=0)
    return jnp.concatenate(left, axis=1), jnp.concatenate([right, jnp.zeros_like(right)], axis=1)


def issue(source, held, jobs, accs):
    slots = jobs[0][2]
    for p in range(slots // 2):
        for unit, job in enumerate(jobs):
            left, right = slot_pair(source, held, job, p)
            pltpu.matmul_push_rhs(right, staging_register=p % 2, mxu_index=unit)
            pltpu.matmul_acc_lhs(accs[unit], left, load_staged_rhs=p % 2)


def one_hot(blocks, kinds, own, count):
    spot = lax.broadcasted_iota(jnp.int32, (own, 128), 0)
    kind = lax.broadcasted_iota(jnp.int32, (count, 128), 0)
    left, right = [], []
    for r in range(8):
        left.append(jnp.where(blocks[r:r + 1] == spot, 1.0, 0.0).astype(jnp.bfloat16))
        right.append(jnp.where(kinds[r:r + 1] == kind, 1.0, 0.0).astype(jnp.bfloat16))
    return left, right


def slot_lanes(parts, slots):
    found = [[], []]
    for table, shift, there, first, width in parts:
        targets = table.shape[1]
        live = (lax.broadcasted_iota(jnp.int32, (slots, targets), 0) < table[2 * slots:2 * slots + 1]) & there
        blocks = jnp.where(live, table[slots:2 * slots] - shift, -1)
        for rows, lanes in ((blocks, found[0]), (table[0:slots], found[1])):
            lanes += [rows[8 * p:8 * p + 8, first:first + width] for p in range(slots // 8)]
    used = sum(a.shape[1] for a in found[0])
    blank = [jnp.full((8, 128 - used), -1, jnp.int32)] if used < 128 else []
    return [jnp.concatenate(lanes + blank, axis=1) for lanes in found]


def main_kernel(bands, mems, edge, *refs):
    source = refs[19]
    own, columns, tile = source.shape
    wide = 2 * tile
    shapes = [(columns, wide)] * RING + [(own, wide), (2 * 8, wide)]

    def scoped(*accs):
        half = len(shapes)
        main_body(bands, mems, edge, accs[:half], accs[half:], *refs)

    pl.run_scoped(
        scoped, *[pltpu.ACC(unit)(shape, jnp.float32) for unit in (0, 1) for shape in shapes]
    )


def main_body(
    bands, mems, edge, first_accs, second_accs,
    fields, mask_h, area_h, target_area_h, tiles, tile_h, block_h, live_h,
    raw, totals, fix_ref,
    mask, area, target_area, table_v, table_s, near_v, near_s,
    stage, source, held, made, came, rows, landed, source_sum, target_sum, tile_sum, uses, coef,
    load_sem, small_sem, near_sem, table_send, table_recv, edge_send, edge_recv, row_send, row_recv, token,
):
    band, mem = lax.axis_index("band"), lax.axis_index("mem")
    count = bands * mems
    me = mem * bands + band
    own, columns, tile = source.shape
    slots, targets = tile_h.shape
    kinds = tiles.shape[0]
    has_low, has_high = band > 0, band < bands - 1
    chunk = HALO_BLK * tile
    chunks = own // HALO_BLK
    ways = ((0, has_high), (1, has_low))

    def neighbour(way):
        return {"band": band + 1 if way == 0 else band - 1}

    barrier = pltpu.get_barrier_semaphore()
    for way, there in ways:
        @pl.when(there)
        def _(way=way):
            pl.semaphore_signal(barrier, inc=1, device_id=neighbour(way), device_id_type=MESH)
    for step in range(1, mems):
        pl.semaphore_signal(
            barrier, inc=1, device_id={"mem": lax.rem(mem + step, mems)}, device_id_type=MESH
        )

    loads = [
        pltpu.make_async_copy(
            fields.at[:, :, pl.ds(c * chunk, chunk)],
            stage.at[:, :, pl.ds(c * chunk, chunk)],
            load_sem.at[c],
        )
        for c in range(chunks)
    ]
    lists = ((tile_h, pl.ds(0, slots)), (block_h, pl.ds(slots, slots)), (live_h, pl.ds(2 * slots, 1)))
    small = [
        pltpu.make_async_copy(a, b, small_sem.at[i])
        for i, (a, b) in enumerate(
            [(a, table_v.at[at]) for a, at in lists]
            + [(mask_h, mask), (area_h, area)]
            + [(a, table_s.at[at]) for a, at in lists]
            + [(tiles, held.at[pl.ds(0, kinds)]), (target_area_h, target_area)]
        )
    ]
    for copy in small[:5]:
        copy.start()
    for c in range(2):
        loads[c].start()
    for copy in small[5:]:
        copy.start()
    for c in range(2, chunks):
        loads[c].start()

    def stand_in(way):
        return [
            pltpu.make_async_copy(a, b.at[way, at], near_sem.at[way, i])
            for i, (a, b, at) in enumerate(
                [(a, near_v, at) for a, at in lists] + [(a, near_s, at) for a, at in lists]
            )
        ]

    for way, there in ways:
        @pl.when(jnp.logical_not(there))
        def _(way=way):
            for copy in stand_in(way):
                copy.start()

    def table_copies(way):
        return [
            pltpu.make_async_remote_copy(
                src_ref=table_v,
                dst_ref=theirs.at[1 - way],
                send_sem=table_send.at[way, i],
                recv_sem=table_recv.at[1 - way, i],
                device_id=neighbour(way),
                device_id_type=MESH,
            )
            for i, theirs in enumerate((near_s, near_v))
        ]

    def edge_copy(way, j):
        return pltpu.make_async_remote_copy(
            src_ref=made.at[way, j],
            dst_ref=came.at[way, j],
            send_sem=edge_send.at[way, j],
            recv_sem=edge_recv.at[way, j],
            device_id=neighbour(way),
            device_id_type=MESH,
        )

    held[kinds] = jnp.zeros((tile, tile), held.dtype)
    source_sum[...] = jnp.zeros((columns, tile), jnp.float32)
    target_sum[...] = jnp.zeros((columns, tile), jnp.float32)

    def weigh_block(n):
        at = pl.ds(n * tile if isinstance(n, int) else pl.multiple_of(n * tile, tile), tile)
        scale = area[:, at] * mask[:, at].astype(jnp.float32)
        part = stage[:, :, at].astype(jnp.float32).reshape(columns, tile) * scale
        source[n] = part.astype(source.dtype)

    def weigh(c):
        def one(n, carry):
            weigh_block(n)
            return carry

        loads[c].wait()
        lax.fori_loop(c * HALO_BLK, (c + 1) * HALO_BLK, one, 0, unroll=8)

    def token_step(up, down):
        for way, at, first in ((0, up, band == 0), (1, down, band == bands - 1)):
            there = has_high if way == 0 else has_low

            @pl.when(at & jnp.logical_not(first))
            def _(way=way):
                pl.semaphore_wait(token.at[way], 1)

            @pl.when(at & there)
            def _(way=way):
                pl.semaphore_signal(
                    token.at[way], inc=1, device_id=neighbour(way), device_id_type=MESH
                )

    for copy in small[3:5]:
        copy.wait()
    weigh(0)
    for copy in small[:3]:
        copy.wait()
    pl.semaphore_wait(
        barrier, has_low.astype(jnp.int32) + has_high.astype(jnp.int32) + (mems - 1)
    )
    for way, there in ways:
        @pl.when(there)
        def _(way=way):
            for copy in table_copies(way):
                copy.start()
    token_step(band == 0, band == bands - 1)
    weigh(1)
    token_step(band == 1, band == bands - 2)

    rings = list(zip(first_accs[:RING], second_accs[:RING]))
    count_accs = (first_accs[RING], second_accs[RING])
    small_accs = (first_accs[RING + 1], second_accs[RING + 1])

    def own_pair(t):
        def sink(values):
            for u, value in enumerate(values):
                at = pl.ds(pl.multiple_of((t + u) * tile, tile), tile)
                raw[t + u] = value * (1.0 / target_area[:, at])

        return [(table_s, t + u, slots, HALO_BLK, 0, own) for u in (0, 1)], sink

    reaches = (
        (HALO_BLK - own, own - HALO_BLK, own),
        (HALO_BLK + own, 0, HALO_BLK),
    )
    firsts = (0, targets - edge)

    def edge_pair(j):
        def sink(values):
            for way, value in enumerate(values):
                made[way, j] = value.astype(made.dtype)

        return [(near_s.at[way], firsts[way] + j, slots, *reaches[way]) for way in (0, 1)], sink

    def stream(pairs, between=()):
        ready = None
        for i, (jobs, sink) in enumerate(pairs):
            issue(source, held, jobs, rings[i % RING])
            if ready is not None:
                ready[1]([pltpu.matmul_pop(acc)[:, :tile] for acc in ready[0]])
            ready = (rings[i % RING], sink)
            if i < len(between):
                between[i]()
        ready[1]([pltpu.matmul_pop(acc)[:, :tile] for acc in ready[0]])

    def tile_sums():
        lane = lax.broadcasted_iota(jnp.int32, (16, 2 * tile), 1)
        line = lax.broadcasted_iota(jnp.int32, (16, 2 * tile), 0)
        ones = jnp.where(lane // tile == line, 1.0, 0.0).astype(held.dtype)
        for g in range(kinds // 4):
            unit = g % 2
            four = [held[4 * g + i] for i in range(4)]
            right = jnp.concatenate(
                [jnp.concatenate(four[:2], axis=1), jnp.concatenate(four[2:], axis=1)], axis=0
            )
            pltpu.matmul_push_rhs(right, staging_register=0, mxu_index=unit, transpose=True)
            pltpu.matmul_acc_lhs(small_accs[unit], ones, load_staged_rhs=0)
            sums = pltpu.matmul_pop(small_accs[unit])
            for i in range(4):
                half = i // 2
                tile_sum[4 * g + i:4 * g + i + 1, :] = sums[i % 2:i % 2 + 1, half * tile:(half + 1) * tile]

    def count_uses(parts):
        left, right = one_hot(*slot_lanes(parts, slots), own, kinds)
        blank = jnp.zeros((2 * tile - 6 * kinds, 2 * tile), held.dtype)
        for r in range(0, 8, 2):
            unit = (r // 2) % 2
            marks = jnp.concatenate(right[r:r + 2], axis=1)
            pltpu.matmul_push_rhs(
                jnp.concatenate([marks] * 6 + [blank], axis=0),
                staging_register=0, mxu_index=unit, transpose=True,
            )
            pltpu.matmul_acc_lhs(
                count_accs[unit], jnp.concatenate(left[r:r + 2], axis=1), load_staged_rhs=0
            )

    def use_counts(add):
        found = (pltpu.matmul_pop(count_accs[0]) + pltpu.matmul_pop(count_accs[1]))[:, :tile]
        found = found + uses[...] if add else found
        uses[...] = found
        high = jnp.floor(found * (1.0 / 256.0)) * 256.0
        lane = lax.broadcasted_iota(jnp.int32, found.shape, 1)
        left = jnp.where(lane < 3 * kinds, found - high, high).astype(held.dtype)
        rest, pieces = tile_sum[...], []
        for _ in range(3):
            pieces.append(rest.astype(held.dtype))
            rest = rest - pieces[-1].astype(jnp.float32)
        right = jnp.concatenate(
            pieces * 2 + [jnp.zeros((2 * tile - 6 * kinds, tile), held.dtype)], axis=0
        )
        pltpu.matmul_push_rhs(
            jnp.concatenate([right, jnp.zeros_like(right)], axis=1), staging_register=0, mxu_index=0
        )
        pltpu.matmul_acc_lhs(
            count_accs[0], jnp.concatenate([left, jnp.zeros_like(left)], axis=1), load_staged_rhs=0
        )

    def keep_coef():
        coef[...] = pltpu.matmul_pop(count_accs[0])[:, :tile]

    def sum_blocks(first, number):
        plain, scaled = source_sum[...], target_sum[...]
        for n in range(first, first + number):
            part = source[n].astype(jnp.float32)
            plain = plain + part
            scaled = scaled + part * coef[n:n + 1, :]
        source_sum[...] = plain
        target_sum[...] = scaled

    for copy in small[5:]:
        copy.wait()
    for c in range(2, chunks):
        loads[c].wait()
    tile_sums()
    count_uses([(table_v[...], HALO_BLK, True, 0, targets)])
    early = EARLY
    lots = early // 2
    fresh = list(range(2 * HALO_BLK, own))
    share = -(-len(fresh) // (lots - 1))

    def beside(i):
        for n in fresh[i * share:(i + 1) * share]:
            weigh_block(n)
        if i == 0:
            use_counts(False)
        if i == 1:
            keep_coef()
        if i == lots - 1:
            sum_blocks(HALO_BLK, own - 2 * HALO_BLK)

    stream(
        [own_pair(t) for t in range(0, early, 2)],
        [functools.partial(beside, i) for i in range(lots)],
    )

    for way, there in ways:
        @pl.when(there)
        def _(way=way):
            for copy in table_copies(1 - way):
                copy.wait_recv()

        @pl.when(jnp.logical_not(there))
        def _(way=way):
            for copy in stand_in(way):
                copy.wait()

    token_step(band == 2, band == bands - 3)

    def send_edge(j):
        for way, there in ways:
            @pl.when(there)
            def _(way=way):
                edge_copy(way, j).start()

    stream([edge_pair(0)])
    send_edge(0)

    near = [(near_v[way], reaches[way][0], there, firsts[way], edge) for way, there in ways]

    def last_sums():
        keep_coef()
        sum_blocks(0, HALO_BLK)

    done = early
    stream(
        [edge_pair(1), edge_pair(2), own_pair(done), own_pair(done + 2)],
        (
            lambda: count_uses(near),
            lambda: use_counts(True),
            last_sums,
            lambda: sum_blocks(own - HALO_BLK, HALO_BLK),
        ),
    )
    send_edge(1)
    send_edge(2)
    done += 4

    rows[0:1, :] = row_of(source_sum[...])
    rows[1:2, :] = row_of(target_sum[...])
    rows[2:3, :] = jnp.broadcast_to(
        jnp.sum(target_area[...], axis=1, keepdims=True), (1, columns)
    )
    rows[3:8, :] = jnp.zeros((5, columns), jnp.float32)

    def place(step):
        other = lax.rem(me + step, count)
        return {"mem": other // bands, "band": lax.rem(other, bands)}

    def row_copy(step):
        return pltpu.make_async_remote_copy(
            src_ref=rows,
            dst_ref=landed.at[step],
            send_sem=row_send.at[step],
            recv_sem=row_recv.at[step],
            device_id=place(step),
            device_id_type=MESH,
        )

    def begin(step, carry):
        row_copy(step).start()
        return carry

    def end(step, carry):
        row_copy(step).wait()
        return carry

    token_step(band > 2, band < bands - 3)
    lax.fori_loop(1, count, begin, 0)
    landed[0] = rows[...]

    steps = (edge - 4) // 2

    def two_edges(i, carry):
        j, t = 3 + 2 * i, done + 2 * i
        stream([edge_pair(j), edge_pair(j + 1), own_pair(t)])
        send_edge(j)
        send_edge(j + 1)
        return carry

    lax.fori_loop(0, steps, two_edges, 0)
    last = done + 2 * steps
    stream([edge_pair(j) for j in range(3 + 2 * steps, edge)] + [own_pair(last)])
    for j in range(3 + 2 * steps, edge):
        send_edge(j)
    last += 2
    stream([own_pair(t) for t in range(last, targets, 2)])

    for way, there in ways:
        @pl.when(there)
        def _(way=way):
            for copy in table_copies(way):
                copy.wait_send()

    lax.fori_loop(1, count, end, 0)
    for m in range(mems):
        total = jnp.zeros(rows.shape, jnp.float32)
        for b in range(bands):
            total = total + landed[lax.rem(me - (m * bands + b) + count, count)]
        totals[m] = total
    mine = totals[mem]
    fix = (mine[0:1, :] - mine[1:2, :]) / mine[2:3, :]
    fix_ref[...] = jnp.broadcast_to(fix, (fix_ref.shape[1], fix.shape[1])).T

    def add(j, carry):
        for way, there in ((0, has_low), (1, has_high)):
            @pl.when(there)
            def _(way=way):
                edge_copy(way, j).wait_recv()
                t = j if way == 0 else targets - edge + j
                at = pl.ds(pl.multiple_of(t * tile, tile), tile)
                share = 1.0 / target_area[:, at]
                raw[t] = raw[t] + came[way, j].astype(jnp.float32) * share
        return carry

    lax.fori_loop(0, edge, add, 0)

    for way, there in ways:
        @pl.when(there)
        def _(way=way):
            def sent(j, carry):
                edge_copy(way, j).wait_send()
                return carry

            lax.fori_loop(0, edge, sent, 0)


def main_call(fields, mask, area, target_area, tiles, tile_t, block_t, live):
    bands, mems = lax.axis_size("band"), lax.axis_size("mem")
    rows, snaps, cells = fields.shape
    columns = rows * snaps
    slots, targets = tile_t.shape
    count, tile = tiles.shape[0], tiles.shape[1]
    own = cells // tile
    edge = HALO_BLK // (own // targets)
    dma = pltpu.SemaphoreType.DMA
    peers = bands * mems
    lines = 2 * slots + 1
    return pl.pallas_call(
        functools.partial(main_kernel, bands, mems, edge),
        in_specs=[HBM] * 8,
        out_specs=(VMEM, VMEM, VMEM),
        out_shape=(
            jax.ShapeDtypeStruct((targets, columns, tile), jnp.float32),
            jax.ShapeDtypeStruct((mems, 8, columns), jnp.float32),
            jax.ShapeDtypeStruct((columns, tile), jnp.float32),
        ),
        scratch_shapes=[
            pltpu.VMEM(mask.shape, mask.dtype),
            pltpu.VMEM(area.shape, area.dtype),
            pltpu.VMEM(target_area.shape, target_area.dtype),
            pltpu.VMEM((lines, targets), jnp.int32),
            pltpu.SMEM((lines, targets), jnp.int32),
            pltpu.VMEM((2, lines, targets), jnp.int32),
            pltpu.SMEM((2, lines, targets), jnp.int32),
            pltpu.VMEM(fields.shape, fields.dtype),
            pltpu.VMEM((own, columns, tile), jnp.bfloat16),
            pltpu.VMEM((count + 1, tile, tile), tiles.dtype),
            pltpu.VMEM((2, edge, columns, tile), SEND_TYPE),
            pltpu.VMEM((2, edge, columns, tile), SEND_TYPE),
            pltpu.VMEM((8, columns), jnp.float32),
            pltpu.VMEM((peers, 8, columns), jnp.float32),
            pltpu.VMEM((columns, tile), jnp.float32),
            pltpu.VMEM((columns, tile), jnp.float32),
            pltpu.VMEM((count, tile), jnp.float32),
            pltpu.VMEM((own, tile), jnp.float32),
            pltpu.VMEM((own, tile), jnp.float32),
            dma((own // HALO_BLK,)),
            dma((10,)),
            dma((2, 6)),
            dma((2, 2)),
            dma((2, 2)),
            dma((2, edge)),
            dma((2, edge)),
            dma((peers,)),
            dma((peers,)),
            pltpu.SemaphoreType.REGULAR((2,)),
        ],
        compiler_params=pltpu.CompilerParams(
            collective_id=0, has_side_effects=True, vmem_limit_bytes=32 << 20
        ),
    )(*[pltpu.with_memory_space_constraint(a, pltpu.HBM) for a in (fields, mask, area, target_area, tiles, tile_t, block_t, live)])


def finish_kernel(fields, snaps, raw_ref, fix_ref, totals_ref, out_ref, mean_ref, ensemble_ref):
    count, columns, tile = raw_ref.shape
    fix = fix_ref[...]
    for n in range(count):
        value = raw_ref[n] + fix
        out_ref[:, :, n * tile:(n + 1) * tile] = value.reshape(columns // snaps, snaps, tile)

    @pl.when(pl.program_id(0) == 1)
    def _():
        mems, members = totals_ref.shape[0], mean_ref.shape[0]
        spot = lax.broadcasted_iota(jnp.int32, (columns, tile), 0)
        lane = lax.broadcasted_iota(jnp.int32, (columns, tile), 1)
        chosen = lax.rem(spot, snaps) == lane
        summed = jnp.zeros((fields, snaps), jnp.float32)

        def table(m):
            row = totals_ref[m, 0:1, :] / totals_ref[m, 2:3, :]
            column = jnp.broadcast_to(row, (tile, columns)).T
            spread = jnp.where(chosen, column, 0.0).reshape(columns // snaps, snaps, tile)
            return jnp.sum(spread, axis=1)[:, 0:snaps]

        mine = table(lax.axis_index("mem"))
        for n in range(members):
            mean_ref[n] = mine[n * fields:(n + 1) * fields]
        for m in range(mems):
            all_of = table(m)
            for n in range(members):
                summed = summed + all_of[n * fields:(n + 1) * fields]
        ensemble_ref[...] = summed / (mems * members)


def finish(raw, fix, totals, members, fields, snaps):
    targets, columns, tile = raw.shape
    steps = 2
    part = targets // steps
    rows = members * fields
    return pl.pallas_call(
        functools.partial(finish_kernel, fields, snaps),
        grid=(steps,),
        in_specs=[
            pl.BlockSpec((part, columns, tile), lambda i: (i, 0, 0)),
            pl.BlockSpec((columns, tile), lambda i: (0, 0)),
            pl.BlockSpec(totals.shape, lambda i: (0, 0, 0)),
        ],
        out_specs=(
            pl.BlockSpec((rows, snaps, part * tile), lambda i: (0, 0, i)),
            pl.BlockSpec((members, fields, snaps), lambda i: (0, 0, 0)),
            pl.BlockSpec((fields, snaps), lambda i: (0, 0)),
        ),
        out_shape=(
            jax.ShapeDtypeStruct((rows, snaps, targets * tile), jnp.float32),
            jax.ShapeDtypeStruct((members, fields, snaps), jnp.float32),
            jax.ShapeDtypeStruct((fields, snaps), jnp.float32),
        ),
        compiler_params=pltpu.CompilerParams(vmem_limit_bytes=16 << 20),
    )(raw, fix, totals)


def on_device(
    surface_fields, land_mask, source_area, target_area, weight_tiles, tile_of, block_of, live_slots
):
    members, fields, snaps, cells = surface_fields.shape
    targets = tile_of.shape[0]
    target_cells = target_area.shape[0]
    raw, totals, fix = main_call(
        surface_fields.reshape(members * fields, snaps, cells),
        land_mask.reshape(1, cells),
        source_area.reshape(1, cells),
        target_area.reshape(1, target_cells),
        weight_tiles,
        tile_of.T,
        block_of.T,
        live_slots.reshape(1, targets),
    )
    regridded, conserved, ensemble = finish(raw, fix, totals, members, fields, snaps)
    return regridded.reshape(members, fields, snaps, target_cells), conserved, ensemble


def solution(mesh):
    placed = (
        P(("grp", "mem"), "fld", None, "band"),
        P("band"),
        P("band"),
        P("band"),
        P(),
        P("band", None),
        P("band", None),
        P("band"),
    )
    return jax.shard_map(
        on_device,
        mesh=mesh,
        in_specs=placed,
        out_specs=(
            P(("grp", "mem"), "fld", None, "band"),
            P(("grp", "mem"), "fld", None),
            P(("grp", "fld"), None),
        ),
        check_vma=False,
    )
```

```python
import functools

import jax
import jax.numpy as jnp
from jax import lax
from jax.experimental import pallas as pl
from jax.experimental.pallas import tpu as pltpu
from jax.sharding import PartitionSpec as P

HALO_BLK = 32
RING = 3
EARLY = 8
SEND_TYPE = jnp.bfloat16
MESH = pl.DeviceIdType.MESH
HBM = pl.BlockSpec(memory_space=pltpu.HBM)
VMEM = pl.BlockSpec(memory_space=pltpu.VMEM)


def row_of(sums):
    return jnp.sum(sums.T, axis=0, keepdims=True)


def slot_pair(source, held, job, p):
    table, n, slots, shift, low, high = job
    tile, zero_tile = held.shape[1], held.shape[0] - 1
    left, right = [], []
    for k in (2 * p, 2 * p + 1):
        block = table[slots + k, n] - shift
        keep = (k < table[2 * slots, n]) & (block >= low) & (block < high)
        left.append(source[jnp.where(keep, block, low)])
        right.append(held[jnp.where(keep, table[k, n], zero_tile)])
    right = jnp.concatenate(right, axis=0)
    return jnp.concatenate(left, axis=1), jnp.concatenate([right, jnp.zeros_like(right)], axis=1)


def issue(source, held, jobs, accs):
    slots = jobs[0][2]
    for p in range(slots // 2):
        for unit, job in enumerate(jobs):
            left, right = slot_pair(source, held, job, p)
            pltpu.matmul_push_rhs(right, staging_register=p % 2, mxu_index=unit)
            pltpu.matmul_acc_lhs(accs[unit], left, load_staged_rhs=p % 2)


def one_hot(blocks, kinds, own, count):
    spot = lax.broadcasted_iota(jnp.int32, (own, 128), 0)
    kind = lax.broadcasted_iota(jnp.int32, (count, 128), 0)
    left, right = [], []
    for r in range(8):
        left.append(jnp.where(blocks[r:r + 1] == spot, 1.0, 0.0).astype(jnp.bfloat16))
        right.append(jnp.where(kinds[r:r + 1] == kind, 1.0, 0.0).astype(jnp.bfloat16))
    return left, right


def slot_lanes(parts, slots):
    found = [[], []]
    for table, shift, there, first, width in parts:
        targets = table.shape[1]
        live = (lax.broadcasted_iota(jnp.int32, (slots, targets), 0) < table[2 * slots:2 * slots + 1]) & there
        blocks = jnp.where(live, table[slots:2 * slots] - shift, -1)
        for rows, lanes in ((blocks, found[0]), (table[0:slots], found[1])):
            lanes += [rows[8 * p:8 * p + 8, first:first + width] for p in range(slots // 8)]
    used = sum(a.shape[1] for a in found[0])
    blank = [jnp.full((8, 128 - used), -1, jnp.int32)] if used < 128 else []
    return [jnp.concatenate(lanes + blank, axis=1) for lanes in found]


def main_kernel(bands, mems, edge, *refs):
    source = refs[19]
    own, columns, tile = source.shape
    wide = 2 * tile
    shapes = [(columns, wide)] * RING + [(own, wide), (2 * 8, wide)]

    def scoped(*accs):
        half = len(shapes)
        main_body(bands, mems, edge, accs[:half], accs[half:], *refs)

    pl.run_scoped(
        scoped, *[pltpu.ACC(unit)(shape, jnp.float32) for unit in (0, 1) for shape in shapes]
    )


def main_body(
    bands, mems, edge, first_accs, second_accs,
    fields, mask_h, area_h, target_area_h, tiles, tile_h, block_h, live_h,
    raw, totals, fix_ref,
    mask, area, target_area, table_v, table_s, near_v, near_s,
    stage, source, held, made, came, rows, landed, source_sum, target_sum, tile_sum, uses, coef,
    load_sem, small_sem, near_sem, table_send, table_recv, edge_send, edge_recv, row_send, row_recv, token,
):
    band, mem = lax.axis_index("band"), lax.axis_index("mem")
    count = bands * mems
    me = mem * bands + band
    own, columns, tile = source.shape
    slots, targets = tile_h.shape
    kinds = tiles.shape[0]
    has_low, has_high = band > 0, band < bands - 1
    chunk = HALO_BLK * tile
    chunks = own // HALO_BLK
    ways = ((0, has_high), (1, has_low))

    def neighbour(way):
        return {"band": band + 1 if way == 0 else band - 1}

    barrier = pltpu.get_barrier_semaphore()
    for way, there in ways:
        @pl.when(there)
        def _(way=way):
            pl.semaphore_signal(barrier, inc=1, device_id=neighbour(way), device_id_type=MESH)
    for step in range(1, mems):
        pl.semaphore_signal(
            barrier, inc=1, device_id={"mem": lax.rem(mem + step, mems)}, device_id_type=MESH
        )

    loads = [
        pltpu.make_async_copy(
            fields.at[:, :, pl.ds(c * chunk, chunk)],
            stage.at[:, :, pl.ds(c * chunk, chunk)],
            load_sem.at[c],
        )
        for c in range(chunks)
    ]
    lists = ((tile_h, pl.ds(0, slots)), (block_h, pl.ds(slots, slots)), (live_h, pl.ds(2 * slots, 1)))
    small = [
        pltpu.make_async_copy(a, b, small_sem.at[i])
        for i, (a, b) in enumerate(
            [(a, table_v.at[at]) for a, at in lists]
            + [(tiles, held.at[pl.ds(0, kinds)]), (mask_h, mask), (area_h, area)]
            + [(a, table_s.at[at]) for a, at in lists]
            + [(target_area_h, target_area)]
        )
    ]
    for copy in small[:6]:
        copy.start()
    for c in range(2):
        loads[c].start()
    for copy in small[6:]:
        copy.start()
    for c in range(2, chunks):
        loads[c].start()

    def stand_in(way):
        return [
            pltpu.make_async_copy(a, b.at[way, at], near_sem.at[way, i])
            for i, (a, b, at) in enumerate(
                [(a, near_v, at) for a, at in lists] + [(a, near_s, at) for a, at in lists]
            )
        ]

    for way, there in ways:
        @pl.when(jnp.logical_not(there))
        def _(way=way):
            for copy in stand_in(way):
                copy.start()

    def table_copies(way):
        return [
            pltpu.make_async_remote_copy(
                src_ref=table_v,
                dst_ref=theirs.at[1 - way],
                send_sem=table_send.at[way, i],
                recv_sem=table_recv.at[1 - way, i],
                device_id=neighbour(way),
                device_id_type=MESH,
            )
            for i, theirs in enumerate((near_s, near_v))
        ]

    def edge_copy(way, j):
        return pltpu.make_async_remote_copy(
            src_ref=made.at[way, j],
            dst_ref=came.at[way, j],
            send_sem=edge_send.at[way, j],
            recv_sem=edge_recv.at[way, j],
            device_id=neighbour(way),
            device_id_type=MESH,
        )

    held[kinds] = jnp.zeros((tile, tile), held.dtype)
    source_sum[...] = jnp.zeros((columns, tile), jnp.float32)
    target_sum[...] = jnp.zeros((columns, tile), jnp.float32)

    def weigh_block(n):
        at = pl.ds(n * tile if isinstance(n, int) else pl.multiple_of(n * tile, tile), tile)
        scale = area[:, at] * mask[:, at].astype(jnp.float32)
        part = stage[:, :, at].astype(jnp.float32).reshape(columns, tile) * scale
        source[n] = part.astype(source.dtype)

    def weigh(c):
        def one(n, carry):
            weigh_block(n)
            return carry

        loads[c].wait()
        lax.fori_loop(c * HALO_BLK, (c + 1) * HALO_BLK, one, 0, unroll=8)

    def token_step(up, down):
        for way, at, first in ((0, up, band == 0), (1, down, band == bands - 1)):
            there = has_high if way == 0 else has_low

            @pl.when(at & jnp.logical_not(first))
            def _(way=way):
                pl.semaphore_wait(token.at[way], 1)

            @pl.when(at & there)
            def _(way=way):
                pl.semaphore_signal(
                    token.at[way], inc=1, device_id=neighbour(way), device_id_type=MESH
                )

    rings = list(zip(first_accs[:RING], second_accs[:RING]))
    count_accs = (first_accs[RING], second_accs[RING])
    small_accs = (first_accs[RING + 1], second_accs[RING + 1])

    def own_pair(t):
        def sink(values):
            for u, value in enumerate(values):
                at = pl.ds(pl.multiple_of((t + u) * tile, tile), tile)
                raw[t + u] = value * (1.0 / target_area[:, at])

        return [(table_s, t + u, slots, HALO_BLK, 0, own) for u in (0, 1)], sink

    reaches = (
        (HALO_BLK - own, own - HALO_BLK, own),
        (HALO_BLK + own, 0, HALO_BLK),
    )
    firsts = (0, targets - edge)

    def edge_pair(j):
        def sink(values):
            for way, value in enumerate(values):
                made[way, j] = value.astype(made.dtype)

        return [(near_s.at[way], firsts[way] + j, slots, *reaches[way]) for way in (0, 1)], sink

    state = {"ready": None, "number": 0}

    def read_out():
        accs, sink = state["ready"]
        sink([pltpu.matmul_pop(acc)[:, :tile] for acc in accs])

    def put(pair):
        jobs, sink = pair
        accs = rings[state["number"] % RING]
        issue(source, held, jobs, accs)
        if state["ready"] is not None:
            read_out()
        state["ready"], state["number"] = (accs, sink), state["number"] + 1

    def tile_sums():
        lane = lax.broadcasted_iota(jnp.int32, (16, 2 * tile), 1)
        line = lax.broadcasted_iota(jnp.int32, (16, 2 * tile), 0)
        ones = jnp.where(lane // tile == line, 1.0, 0.0).astype(held.dtype)
        for g in range(kinds // 4):
            unit = g % 2
            four = [held[4 * g + i] for i in range(4)]
            right = jnp.concatenate(
                [jnp.concatenate(four[:2], axis=1), jnp.concatenate(four[2:], axis=1)], axis=0
            )
            pltpu.matmul_push_rhs(right, staging_register=0, mxu_index=unit, transpose=True)
            pltpu.matmul_acc_lhs(small_accs[unit], ones, load_staged_rhs=0)
            sums = pltpu.matmul_pop(small_accs[unit])
            for i in range(4):
                half = i // 2
                tile_sum[4 * g + i:4 * g + i + 1, :] = sums[i % 2:i % 2 + 1, half * tile:(half + 1) * tile]

    def count_uses(parts):
        left, right = one_hot(*slot_lanes(parts, slots), own, kinds)
        blank = jnp.zeros((2 * tile - 6 * kinds, 2 * tile), held.dtype)
        for r in range(0, 8, 2):
            unit = (r // 2) % 2
            marks = jnp.concatenate(right[r:r + 2], axis=1)
            pltpu.matmul_push_rhs(
                jnp.concatenate([marks] * 6 + [blank], axis=0),
                staging_register=0, mxu_index=unit, transpose=True,
            )
            pltpu.matmul_acc_lhs(
                count_accs[unit], jnp.concatenate(left[r:r + 2], axis=1), load_staged_rhs=0
            )

    def use_counts(add):
        found = (pltpu.matmul_pop(count_accs[0]) + pltpu.matmul_pop(count_accs[1]))[:, :tile]
        found = found + uses[...] if add else found
        uses[...] = found
        high = jnp.floor(found * (1.0 / 256.0)) * 256.0
        lane = lax.broadcasted_iota(jnp.int32, found.shape, 1)
        left = jnp.where(lane < 3 * kinds, found - high, high).astype(held.dtype)
        rest, pieces = tile_sum[...], []
        for _ in range(3):
            pieces.append(rest.astype(held.dtype))
            rest = rest - pieces[-1].astype(jnp.float32)
        right = jnp.concatenate(
            pieces * 2 + [jnp.zeros((2 * tile - 6 * kinds, tile), held.dtype)], axis=0
        )
        pltpu.matmul_push_rhs(
            jnp.concatenate([right, jnp.zeros_like(right)], axis=1), staging_register=0, mxu_index=0
        )
        pltpu.matmul_acc_lhs(
            count_accs[0], jnp.concatenate([left, jnp.zeros_like(left)], axis=1), load_staged_rhs=0
        )

    def keep_coef():
        coef[...] = pltpu.matmul_pop(count_accs[0])[:, :tile]

    def sum_blocks(first, number):
        plain, scaled = source_sum[...], target_sum[...]
        for n in range(first, first + number):
            part = source[n].astype(jnp.float32)
            plain = plain + part
            scaled = scaled + part * coef[n:n + 1, :]
        source_sum[...] = plain
        target_sum[...] = scaled

    def enter():
        pl.semaphore_wait(
            barrier, has_low.astype(jnp.int32) + has_high.astype(jnp.int32) + (mems - 1)
        )
        for way, there in ways:
            @pl.when(there)
            def _(way=way):
                for copy in table_copies(way):
                    copy.start()
        token_step(band == 0, band == bands - 1)

    for copy in small[:3]:
        copy.wait()

    enter()

    small[3].wait()
    tile_sums()
    count_uses([(table_v[...], HALO_BLK, True, 0, targets)])
    use_counts(False)
    keep_coef()
    for copy in small[4:6]:
        copy.wait()
    weigh(0)
    for c in range(1, chunks):
        weigh(c)
    token_step(band == 1, band == bands - 2)

    for copy in small[6:]:
        copy.wait()
    early = EARLY
    for t in range(0, early, 2):
        put(own_pair(t))
        if t == 0:
            sum_blocks(HALO_BLK, own - 2 * HALO_BLK)

    for way, there in ways:
        @pl.when(there)
        def _(way=way):
            for copy in table_copies(1 - way):
                copy.wait_recv()

        @pl.when(jnp.logical_not(there))
        def _(way=way):
            for copy in stand_in(way):
                copy.wait()


    token_step(band == 2, band == bands - 3)

    def send_edge(j):
        for way, there in ways:
            @pl.when(there)
            def _(way=way):
                edge_copy(way, j).start()

    near = [(near_v[way], reaches[way][0], there, firsts[way], edge) for way, there in ways]
    put(edge_pair(0))
    count_uses(near)
    put(edge_pair(1))
    use_counts(True)
    send_edge(0)
    put(edge_pair(2))
    keep_coef()
    sum_blocks(0, HALO_BLK)
    send_edge(1)
    put(own_pair(early))
    sum_blocks(own - HALO_BLK, HALO_BLK)
    send_edge(2)
    put(edge_pair(3))
    rows[0:1, :] = row_of(source_sum[...])
    rows[1:2, :] = row_of(target_sum[...])
    rows[2:3, :] = jnp.broadcast_to(
        jnp.sum(target_area[...], axis=1, keepdims=True), (1, columns)
    )
    rows[3:8, :] = jnp.zeros((5, columns), jnp.float32)

    def place(step):
        other = lax.rem(me + step, count)
        return {"mem": other // bands, "band": lax.rem(other, bands)}

    def row_copy(step):
        return pltpu.make_async_remote_copy(
            src_ref=rows,
            dst_ref=landed.at[step],
            send_sem=row_send.at[step],
            recv_sem=row_recv.at[step],
            device_id=place(step),
            device_id_type=MESH,
        )

    def begin(step, carry):
        row_copy(step).start()
        return carry

    def end(step, carry):
        row_copy(step).wait()
        return carry

    token_step(band > 2, band < bands - 3)
    lax.fori_loop(1, count, begin, 0)
    landed[0] = rows[...]

    for j in range(4, edge):
        put(edge_pair(j))
        send_edge(j - 1)
    for t in range(early + 2, targets, 2):
        put(own_pair(t))
        if t == early + 2:
            send_edge(edge - 1)
    read_out()

    for way, there in ways:
        @pl.when(there)
        def _(way=way):
            for copy in table_copies(way):
                copy.wait_send()

    lax.fori_loop(1, count, end, 0)
    for m in range(mems):
        total = jnp.zeros(rows.shape, jnp.float32)
        for b in range(bands):
            total = total + landed[lax.rem(me - (m * bands + b) + count, count)]
        totals[m] = total
    mine = totals[mem]
    fix = (mine[0:1, :] - mine[1:2, :]) / mine[2:3, :]
    fix_ref[...] = jnp.broadcast_to(fix, (fix_ref.shape[1], fix.shape[1])).T

    def add(j, carry):
        for way, there in ((0, has_low), (1, has_high)):
            @pl.when(there)
            def _(way=way):
                edge_copy(way, j).wait_recv()
                t = j if way == 0 else targets - edge + j
                at = pl.ds(pl.multiple_of(t * tile, tile), tile)
                share = 1.0 / target_area[:, at]
                raw[t] = raw[t] + came[way, j].astype(jnp.float32) * share
        return carry

    lax.fori_loop(0, edge, add, 0)

    for way, there in ways:
        @pl.when(there)
        def _(way=way):
            def sent(j, carry):
                edge_copy(way, j).wait_send()
                return carry

            lax.fori_loop(0, edge, sent, 0)


def main_call(fields, mask, area, target_area, tiles, tile_t, block_t, live):
    bands, mems = lax.axis_size("band"), lax.axis_size("mem")
    rows, snaps, cells = fields.shape
    columns = rows * snaps
    slots, targets = tile_t.shape
    count, tile = tiles.shape[0], tiles.shape[1]
    own = cells // tile
    edge = HALO_BLK // (own // targets)
    dma = pltpu.SemaphoreType.DMA
    peers = bands * mems
    lines = 2 * slots + 1
    return pl.pallas_call(
        functools.partial(main_kernel, bands, mems, edge),
        in_specs=[HBM] * 8,
        out_specs=(VMEM, VMEM, VMEM),
        out_shape=(
            jax.ShapeDtypeStruct((targets, columns, tile), jnp.float32),
            jax.ShapeDtypeStruct((mems, 8, columns), jnp.float32),
            jax.ShapeDtypeStruct((columns, tile), jnp.float32),
        ),
        scratch_shapes=[
            pltpu.VMEM(mask.shape, mask.dtype),
            pltpu.VMEM(area.shape, area.dtype),
            pltpu.VMEM(target_area.shape, target_area.dtype),
            pltpu.VMEM((lines, targets), jnp.int32),
            pltpu.SMEM((lines, targets), jnp.int32),
            pltpu.VMEM((2, lines, targets), jnp.int32),
            pltpu.SMEM((2, lines, targets), jnp.int32),
            pltpu.VMEM(fields.shape, fields.dtype),
            pltpu.VMEM((own, columns, tile), jnp.bfloat16),
            pltpu.VMEM((count + 1, tile, tile), tiles.dtype),
            pltpu.VMEM((2, edge, columns, tile), SEND_TYPE),
            pltpu.VMEM((2, edge, columns, tile), SEND_TYPE),
            pltpu.VMEM((8, columns), jnp.float32),
            pltpu.VMEM((peers, 8, columns), jnp.float32),
            pltpu.VMEM((columns, tile), jnp.float32),
            pltpu.VMEM((columns, tile), jnp.float32),
            pltpu.VMEM((count, tile), jnp.float32),
            pltpu.VMEM((own, tile), jnp.float32),
            pltpu.VMEM((own, tile), jnp.float32),
            dma((own // HALO_BLK,)),
            dma((10,)),
            dma((2, 6)),
            dma((2, 2)),
            dma((2, 2)),
            dma((2, edge)),
            dma((2, edge)),
            dma((peers,)),
            dma((peers,)),
            pltpu.SemaphoreType.REGULAR((2,)),
        ],
        compiler_params=pltpu.CompilerParams(
            collective_id=0, has_side_effects=True, vmem_limit_bytes=32 << 20
        ),
    )(*[pltpu.with_memory_space_constraint(a, pltpu.HBM) for a in (fields, mask, area, target_area, tiles, tile_t, block_t, live)])


def finish_kernel(fields, snaps, raw_ref, fix_ref, totals_ref, out_ref, mean_ref, ensemble_ref):
    count, columns, tile = raw_ref.shape
    fix = fix_ref[...]
    for n in range(count):
        value = raw_ref[n] + fix
        out_ref[:, :, n * tile:(n + 1) * tile] = value.reshape(columns // snaps, snaps, tile)

    @pl.when(pl.program_id(0) == 1)
    def _():
        mems, members = totals_ref.shape[0], mean_ref.shape[0]
        spot = lax.broadcasted_iota(jnp.int32, (columns, tile), 0)
        lane = lax.broadcasted_iota(jnp.int32, (columns, tile), 1)
        chosen = lax.rem(spot, snaps) == lane
        summed = jnp.zeros((fields, snaps), jnp.float32)

        def table(m):
            row = totals_ref[m, 0:1, :] / totals_ref[m, 2:3, :]
            column = jnp.broadcast_to(row, (tile, columns)).T
            spread = jnp.where(chosen, column, 0.0).reshape(columns // snaps, snaps, tile)
            return jnp.sum(spread, axis=1)[:, 0:snaps]

        mine = table(lax.axis_index("mem"))
        for n in range(members):
            mean_ref[n] = mine[n * fields:(n + 1) * fields]
        for m in range(mems):
            all_of = table(m)
            for n in range(members):
                summed = summed + all_of[n * fields:(n + 1) * fields]
        ensemble_ref[...] = summed / (mems * members)


def finish(raw, fix, totals, members, fields, snaps):
    targets, columns, tile = raw.shape
    steps = 2
    part = targets // steps
    rows = members * fields
    return pl.pallas_call(
        functools.partial(finish_kernel, fields, snaps),
        grid=(steps,),
        in_specs=[
            pl.BlockSpec((part, columns, tile), lambda i: (i, 0, 0)),
            pl.BlockSpec((columns, tile), lambda i: (0, 0)),
            pl.BlockSpec(totals.shape, lambda i: (0, 0, 0)),
        ],
        out_specs=(
            pl.BlockSpec((rows, snaps, part * tile), lambda i: (0, 0, i)),
            pl.BlockSpec((members, fields, snaps), lambda i: (0, 0, 0)),
            pl.BlockSpec((fields, snaps), lambda i: (0, 0)),
        ),
        out_shape=(
            jax.ShapeDtypeStruct((rows, snaps, targets * tile), jnp.float32),
            jax.ShapeDtypeStruct((members, fields, snaps), jnp.float32),
            jax.ShapeDtypeStruct((fields, snaps), jnp.float32),
        ),
        compiler_params=pltpu.CompilerParams(vmem_limit_bytes=16 << 20),
    )(raw, fix, totals)


def on_device(
    surface_fields, land_mask, source_area, target_area, weight_tiles, tile_of, block_of, live_slots
):
    members, fields, snaps, cells = surface_fields.shape
    targets = tile_of.shape[0]
    target_cells = target_area.shape[0]
    raw, totals, fix = main_call(
        surface_fields.reshape(members * fields, snaps, cells),
        land_mask.reshape(1, cells),
        source_area.reshape(1, cells),
        target_area.reshape(1, target_cells),
        weight_tiles,
        tile_of.T,
        block_of.T,
        live_slots.reshape(1, targets),
    )
    regridded, conserved, ensemble = finish(raw, fix, totals, members, fields, snaps)
    return regridded.reshape(members, fields, snaps, target_cells), conserved, ensemble


def solution(mesh):
    placed = (
        P(("grp", "mem"), "fld", None, "band"),
        P("band"),
        P("band"),
        P("band"),
        P(),
        P("band", None),
        P("band", None),
        P("band"),
    )
    return jax.shard_map(
        on_device,
        mesh=mesh,
        in_specs=placed,
        out_specs=(
            P(("grp", "mem"), "fld", None, "band"),
            P(("grp", "mem"), "fld", None),
            P(("grp", "fld"), None),
        ),
        check_vma=False,
    )
```

```python
import functools

import jax
import jax.numpy as jnp
from jax import lax
from jax.experimental import pallas as pl
from jax.experimental.pallas import tpu as pltpu
from jax.sharding import PartitionSpec as P

HALO_BLK = 32
RING = 3
EARLY = 8
SEND_TYPE = jnp.bfloat16
MESH = pl.DeviceIdType.MESH
HBM = pl.BlockSpec(memory_space=pltpu.HBM)
VMEM = pl.BlockSpec(memory_space=pltpu.VMEM)


def row_of(sums):
    return jnp.sum(sums.T, axis=0, keepdims=True)


def slot_pair(source, held, job, p):
    table, n, slots, shift, low, high = job
    tile, zero_tile = held.shape[1], held.shape[0] - 1
    left, right = [], []
    for k in (2 * p, 2 * p + 1):
        block = table[slots + k, n] - shift
        keep = (k < table[2 * slots, n]) & (block >= low) & (block < high)
        left.append(source[jnp.where(keep, block, low)])
        right.append(held[jnp.where(keep, table[k, n], zero_tile)])
    right = jnp.concatenate(right, axis=0)
    return jnp.concatenate(left, axis=1), jnp.concatenate([right, jnp.zeros_like(right)], axis=1)


def issue(source, held, jobs, accs):
    slots = jobs[0][2]
    for p in range(slots // 2):
        for unit, job in enumerate(jobs):
            left, right = slot_pair(source, held, job, p)
            pltpu.matmul_push_rhs(right, staging_register=p % 2, mxu_index=unit)
            pltpu.matmul_acc_lhs(accs[unit], left, load_staged_rhs=p % 2)


def one_hot(blocks, kinds, own, count):
    spot = lax.broadcasted_iota(jnp.int32, (own, 128), 0)
    kind = lax.broadcasted_iota(jnp.int32, (count, 128), 0)
    left, right = [], []
    for r in range(8):
        left.append(jnp.where(blocks[r:r + 1] == spot, 1.0, 0.0).astype(jnp.bfloat16))
        right.append(jnp.where(kinds[r:r + 1] == kind, 1.0, 0.0).astype(jnp.bfloat16))
    return left, right


def slot_lanes(parts, slots):
    found = [[], []]
    for table, shift, there, first, width in parts:
        targets = table.shape[1]
        live = (lax.broadcasted_iota(jnp.int32, (slots, targets), 0) < table[2 * slots:2 * slots + 1]) & there
        blocks = jnp.where(live, table[slots:2 * slots] - shift, -1)
        for rows, lanes in ((blocks, found[0]), (table[0:slots], found[1])):
            lanes += [rows[8 * p:8 * p + 8, first:first + width] for p in range(slots // 8)]
    used = sum(a.shape[1] for a in found[0])
    blank = [jnp.full((8, 128 - used), -1, jnp.int32)] if used < 128 else []
    return [jnp.concatenate(lanes + blank, axis=1) for lanes in found]


def main_kernel(bands, mems, edge, *refs):
    source = refs[19]
    own, columns, tile = source.shape
    wide = 2 * tile
    shapes = [(columns, wide)] * RING + [(own, wide), (2 * 8, wide)]

    def scoped(*accs):
        half = len(shapes)
        main_body(bands, mems, edge, accs[:half], accs[half:], *refs)

    pl.run_scoped(
        scoped, *[pltpu.ACC(unit)(shape, jnp.float32) for unit in (0, 1) for shape in shapes]
    )


def main_body(
    bands, mems, edge, first_accs, second_accs,
    fields, mask_h, area_h, target_area_h, tiles, tile_h, block_h, live_h,
    raw, totals, fix_ref,
    mask, area, target_area, table_v, table_s, near_v, near_s,
    stage, source, held, made, came, rows, landed, source_sum, target_sum, tile_sum, uses, coef,
    load_sem, small_sem, near_sem, table_send, table_recv, edge_send, edge_recv, row_send, row_recv, token,
):
    band, mem = lax.axis_index("band"), lax.axis_index("mem")
    count = bands * mems
    me = mem * bands + band
    own, columns, tile = source.shape
    slots, targets = tile_h.shape
    kinds = tiles.shape[0]
    has_low, has_high = band > 0, band < bands - 1
    chunk = HALO_BLK * tile
    chunks = own // HALO_BLK
    ways = ((0, has_high), (1, has_low))

    def neighbour(way):
        return {"band": band + 1 if way == 0 else band - 1}

    barrier = pltpu.get_barrier_semaphore()
    for way, there in ways:
        @pl.when(there)
        def _(way=way):
            pl.semaphore_signal(barrier, inc=1, device_id=neighbour(way), device_id_type=MESH)
    for step in range(1, mems):
        pl.semaphore_signal(
            barrier, inc=1, device_id={"mem": lax.rem(mem + step, mems)}, device_id_type=MESH
        )

    loads = [
        pltpu.make_async_copy(
            fields.at[:, :, pl.ds(c * chunk, chunk)],
            stage.at[:, :, pl.ds(c * chunk, chunk)],
            load_sem.at[c],
        )
        for c in range(chunks)
    ]
    lists = ((tile_h, pl.ds(0, slots)), (block_h, pl.ds(slots, slots)), (live_h, pl.ds(2 * slots, 1)))
    small = [
        pltpu.make_async_copy(a, b, small_sem.at[i])
        for i, (a, b) in enumerate(
            [(a, table_v.at[at]) for a, at in lists]
            + [(tiles, held.at[pl.ds(0, kinds)]), (mask_h, mask), (area_h, area)]
            + [(a, table_s.at[at]) for a, at in lists]
            + [(target_area_h, target_area)]
        )
    ]
    for copy in small[:6]:
        copy.start()
    for c in range(2):
        loads[c].start()
    for copy in small[6:]:
        copy.start()
    for c in range(2, chunks):
        loads[c].start()

    def stand_in(way):
        return [
            pltpu.make_async_copy(a, b.at[way, at], near_sem.at[way, i])
            for i, (a, b, at) in enumerate(
                [(a, near_v, at) for a, at in lists] + [(a, near_s, at) for a, at in lists]
            )
        ]

    for way, there in ways:
        @pl.when(jnp.logical_not(there))
        def _(way=way):
            for copy in stand_in(way):
                copy.start()

    def table_copies(way):
        return [
            pltpu.make_async_remote_copy(
                src_ref=table_v,
                dst_ref=theirs.at[1 - way],
                send_sem=table_send.at[way, i],
                recv_sem=table_recv.at[1 - way, i],
                device_id=neighbour(way),
                device_id_type=MESH,
            )
            for i, theirs in enumerate((near_s, near_v))
        ]

    def edge_copy(way, j):
        return pltpu.make_async_remote_copy(
            src_ref=made.at[way, j],
            dst_ref=came.at[way, j],
            send_sem=edge_send.at[way, j],
            recv_sem=edge_recv.at[way, j],
            device_id=neighbour(way),
            device_id_type=MESH,
        )

    held[kinds] = jnp.zeros((tile, tile), held.dtype)
    source_sum[...] = jnp.zeros((columns, tile), jnp.float32)
    target_sum[...] = jnp.zeros((columns, tile), jnp.float32)

    def weigh_block(n):
        at = pl.ds(n * tile if isinstance(n, int) else pl.multiple_of(n * tile, tile), tile)
        scale = area[:, at] * mask[:, at].astype(jnp.float32)
        part = stage[:, :, at].astype(jnp.float32).reshape(columns, tile) * scale
        source[n] = part.astype(source.dtype)

    def weigh(c):
        def one(n, carry):
            weigh_block(n)
            return carry

        loads[c].wait()
        lax.fori_loop(c * HALO_BLK, (c + 1) * HALO_BLK, one, 0, unroll=HALO_BLK)

    def token_step(up, down):
        for way, at, first in ((0, up, band == 0), (1, down, band == bands - 1)):
            there = has_high if way == 0 else has_low

            @pl.when(at & jnp.logical_not(first))
            def _(way=way):
                pl.semaphore_wait(token.at[way], 1)

            @pl.when(at & there)
            def _(way=way):
                pl.semaphore_signal(
                    token.at[way], inc=1, device_id=neighbour(way), device_id_type=MESH
                )

    rings = list(zip(first_accs[:RING], second_accs[:RING]))
    count_accs = (first_accs[RING], second_accs[RING])
    small_accs = (first_accs[RING + 1], second_accs[RING + 1])

    def own_pair(t):
        def sink(values):
            for u, value in enumerate(values):
                at = pl.ds(pl.multiple_of((t + u) * tile, tile), tile)
                raw[t + u] = value * (1.0 / target_area[:, at])

        return [(table_s, t + u, slots, HALO_BLK, 0, own) for u in (0, 1)], sink

    reaches = (
        (HALO_BLK - own, own - HALO_BLK, own),
        (HALO_BLK + own, 0, HALO_BLK),
    )
    firsts = (0, targets - edge)

    def edge_pair(j):
        def sink(values):
            for way, value in enumerate(values):
                made[way, j] = value.astype(made.dtype)

        return [(near_s.at[way], firsts[way] + j, slots, *reaches[way]) for way in (0, 1)], sink

    state = {"ready": None, "number": 0}

    def read_out():
        accs, sink = state["ready"]
        sink([pltpu.matmul_pop(acc)[:, :tile] for acc in accs])

    def put(pair):
        jobs, sink = pair
        accs = rings[state["number"] % RING]
        issue(source, held, jobs, accs)
        if state["ready"] is not None:
            read_out()
        state["ready"], state["number"] = (accs, sink), state["number"] + 1

    def tile_sums():
        lane = lax.broadcasted_iota(jnp.int32, (16, 2 * tile), 1)
        line = lax.broadcasted_iota(jnp.int32, (16, 2 * tile), 0)
        ones = jnp.where(lane // tile == line, 1.0, 0.0).astype(held.dtype)
        for g in range(kinds // 4):
            unit = g % 2
            four = [held[4 * g + i] for i in range(4)]
            right = jnp.concatenate(
                [jnp.concatenate(four[:2], axis=1), jnp.concatenate(four[2:], axis=1)], axis=0
            )
            pltpu.matmul_push_rhs(right, staging_register=0, mxu_index=unit, transpose=True)
            pltpu.matmul_acc_lhs(small_accs[unit], ones, load_staged_rhs=0)
            sums = pltpu.matmul_pop(small_accs[unit])
            for i in range(4):
                half = i // 2
                tile_sum[4 * g + i:4 * g + i + 1, :] = sums[i % 2:i % 2 + 1, half * tile:(half + 1) * tile]

    def count_uses(parts):
        left, right = one_hot(*slot_lanes(parts, slots), own, kinds)
        blank = jnp.zeros((2 * tile - 6 * kinds, 2 * tile), held.dtype)
        for r in range(0, 8, 2):
            unit = (r // 2) % 2
            marks = jnp.concatenate(right[r:r + 2], axis=1)
            pltpu.matmul_push_rhs(
                jnp.concatenate([marks] * 6 + [blank], axis=0),
                staging_register=0, mxu_index=unit, transpose=True,
            )
            pltpu.matmul_acc_lhs(
                count_accs[unit], jnp.concatenate(left[r:r + 2], axis=1), load_staged_rhs=0
            )

    def use_counts(add):
        found = (pltpu.matmul_pop(count_accs[0]) + pltpu.matmul_pop(count_accs[1]))[:, :tile]
        found = found + uses[...] if add else found
        uses[...] = found
        high = jnp.floor(found * (1.0 / 256.0)) * 256.0
        lane = lax.broadcasted_iota(jnp.int32, found.shape, 1)
        left = jnp.where(lane < 3 * kinds, found - high, high).astype(held.dtype)
        rest, pieces = tile_sum[...], []
        for _ in range(3):
            pieces.append(rest.astype(held.dtype))
            rest = rest - pieces[-1].astype(jnp.float32)
        right = jnp.concatenate(
            pieces * 2 + [jnp.zeros((2 * tile - 6 * kinds, tile), held.dtype)], axis=0
        )
        pltpu.matmul_push_rhs(
            jnp.concatenate([right, jnp.zeros_like(right)], axis=1), staging_register=0, mxu_index=0
        )
        pltpu.matmul_acc_lhs(
            count_accs[0], jnp.concatenate([left, jnp.zeros_like(left)], axis=1), load_staged_rhs=0
        )

    def keep_coef():
        coef[...] = pltpu.matmul_pop(count_accs[0])[:, :tile]

    def sum_blocks(first, number):
        plain, scaled = source_sum[...], target_sum[...]
        for n in range(first, first + number):
            part = source[n].astype(jnp.float32)
            plain = plain + part
            scaled = scaled + part * coef[n:n + 1, :]
        source_sum[...] = plain
        target_sum[...] = scaled

    def enter():
        pl.semaphore_wait(
            barrier, has_low.astype(jnp.int32) + has_high.astype(jnp.int32) + (mems - 1)
        )
        for way, there in ways:
            @pl.when(there)
            def _(way=way):
                for copy in table_copies(way):
                    copy.start()
        token_step(band == 0, band == bands - 1)

    for copy in small[:3]:
        copy.wait()

    enter()

    small[3].wait()
    tile_sums()
    count_uses([(table_v[...], HALO_BLK, True, 0, targets)])
    use_counts(False)
    keep_coef()
    for copy in small[4:6]:
        copy.wait()
    weigh(0)
    for c in range(1, chunks):
        weigh(c)
    token_step(band == 1, band == bands - 2)

    for copy in small[6:]:
        copy.wait()
    early = EARLY
    for t in range(0, early, 2):
        put(own_pair(t))
        if t == 0:
            sum_blocks(HALO_BLK, own - 2 * HALO_BLK)

    for way, there in ways:
        @pl.when(there)
        def _(way=way):
            for copy in table_copies(1 - way):
                copy.wait_recv()

        @pl.when(jnp.logical_not(there))
        def _(way=way):
            for copy in stand_in(way):
                copy.wait()


    token_step(band == 2, band == bands - 3)

    def send_edge(j):
        for way, there in ways:
            @pl.when(there)
            def _(way=way):
                edge_copy(way, j).start()

    near = [(near_v[way], reaches[way][0], there, firsts[way], edge) for way, there in ways]
    put(edge_pair(0))
    count_uses(near)
    put(edge_pair(1))
    use_counts(True)
    send_edge(0)
    put(edge_pair(2))
    keep_coef()
    sum_blocks(0, HALO_BLK)
    send_edge(1)
    put(own_pair(early))
    sum_blocks(own - HALO_BLK, HALO_BLK)
    send_edge(2)
    put(edge_pair(3))
    rows[0:1, :] = row_of(source_sum[...])
    rows[1:2, :] = row_of(target_sum[...])
    rows[2:3, :] = jnp.broadcast_to(
        jnp.sum(target_area[...], axis=1, keepdims=True), (1, columns)
    )
    rows[3:8, :] = jnp.zeros((5, columns), jnp.float32)

    def place(step):
        other = lax.rem(me + step, count)
        return {"mem": other // bands, "band": lax.rem(other, bands)}

    def row_copy(step):
        return pltpu.make_async_remote_copy(
            src_ref=rows,
            dst_ref=landed.at[step],
            send_sem=row_send.at[step],
            recv_sem=row_recv.at[step],
            device_id=place(step),
            device_id_type=MESH,
        )

    def begin(step, carry):
        row_copy(step).start()
        return carry

    def end(step, carry):
        row_copy(step).wait()
        return carry

    token_step(band > 2, band < bands - 3)
    lax.fori_loop(1, count, begin, 0)
    landed[0] = rows[...]

    for j in range(4, edge):
        put(edge_pair(j))
        send_edge(j - 1)
    for t in range(early + 2, targets, 2):
        put(own_pair(t))
        if t == early + 2:
            send_edge(edge - 1)
    read_out()

    for way, there in ways:
        @pl.when(there)
        def _(way=way):
            for copy in table_copies(way):
                copy.wait_send()

    lax.fori_loop(1, count, end, 0)
    for m in range(mems):
        total = jnp.zeros(rows.shape, jnp.float32)
        for b in range(bands):
            total = total + landed[lax.rem(me - (m * bands + b) + count, count)]
        totals[m] = total
    mine = totals[mem]
    fix = (mine[0:1, :] - mine[1:2, :]) / mine[2:3, :]
    fix_ref[...] = jnp.broadcast_to(fix, (fix_ref.shape[1], fix.shape[1])).T

    for way, there in ((0, has_low), (1, has_high)):
        @pl.when(there)
        def _(way=way):
            def add(g, carry):
                for j in (2 * g, 2 * g + 1):
                    edge_copy(way, j).wait_recv()
                for j in (2 * g, 2 * g + 1):
                    t = j if way == 0 else targets - edge + j
                    at = pl.ds(pl.multiple_of(t * tile, tile), tile)
                    share = 1.0 / target_area[:, at]
                    raw[t] = raw[t] + came[way, j].astype(jnp.float32) * share
                return carry

            lax.fori_loop(0, edge // 2, add, 0)

    for way, there in ways:
        @pl.when(there)
        def _(way=way):
            def sent(j, carry):
                edge_copy(way, j).wait_send()
                return carry

            lax.fori_loop(0, edge, sent, 0)


def main_call(fields, mask, area, target_area, tiles, tile_t, block_t, live):
    bands, mems = lax.axis_size("band"), lax.axis_size("mem")
    rows, snaps, cells = fields.shape
    columns = rows * snaps
    slots, targets = tile_t.shape
    count, tile = tiles.shape[0], tiles.shape[1]
    own = cells // tile
    edge = HALO_BLK // (own // targets)
    dma = pltpu.SemaphoreType.DMA
    peers = bands * mems
    lines = 2 * slots + 1
    return pl.pallas_call(
        functools.partial(main_kernel, bands, mems, edge),
        in_specs=[HBM] * 8,
        out_specs=(VMEM, VMEM, VMEM),
        out_shape=(
            jax.ShapeDtypeStruct((targets, columns, tile), jnp.float32),
            jax.ShapeDtypeStruct((mems, 8, columns), jnp.float32),
            jax.ShapeDtypeStruct((columns, tile), jnp.float32),
        ),
        scratch_shapes=[
            pltpu.VMEM(mask.shape, mask.dtype),
            pltpu.VMEM(area.shape, area.dtype),
            pltpu.VMEM(target_area.shape, target_area.dtype),
            pltpu.VMEM((lines, targets), jnp.int32),
            pltpu.SMEM((lines, targets), jnp.int32),
            pltpu.VMEM((2, lines, targets), jnp.int32),
            pltpu.SMEM((2, lines, targets), jnp.int32),
            pltpu.VMEM(fields.shape, fields.dtype),
            pltpu.VMEM((own, columns, tile), jnp.bfloat16),
            pltpu.VMEM((count + 1, tile, tile), tiles.dtype),
            pltpu.VMEM((2, edge, columns, tile), SEND_TYPE),
            pltpu.VMEM((2, edge, columns, tile), SEND_TYPE),
            pltpu.VMEM((8, columns), jnp.float32),
            pltpu.VMEM((peers, 8, columns), jnp.float32),
            pltpu.VMEM((columns, tile), jnp.float32),
            pltpu.VMEM((columns, tile), jnp.float32),
            pltpu.VMEM((count, tile), jnp.float32),
            pltpu.VMEM((own, tile), jnp.float32),
            pltpu.VMEM((own, tile), jnp.float32),
            dma((own // HALO_BLK,)),
            dma((10,)),
            dma((2, 6)),
            dma((2, 2)),
            dma((2, 2)),
            dma((2, edge)),
            dma((2, edge)),
            dma((peers,)),
            dma((peers,)),
            pltpu.SemaphoreType.REGULAR((2,)),
        ],
        compiler_params=pltpu.CompilerParams(
            collective_id=0, has_side_effects=True, vmem_limit_bytes=32 << 20
        ),
    )(*[pltpu.with_memory_space_constraint(a, pltpu.HBM) for a in (fields, mask, area, target_area, tiles, tile_t, block_t, live)])


def finish_kernel(fields, snaps, raw_ref, fix_ref, totals_ref, out_ref, mean_ref, ensemble_ref):
    count, columns, tile = raw_ref.shape
    fix = fix_ref[...]
    for n in range(count):
        value = raw_ref[n] + fix
        out_ref[:, :, n * tile:(n + 1) * tile] = value.reshape(columns // snaps, snaps, tile)

    @pl.when(pl.program_id(0) == 1)
    def _():
        mems, members = totals_ref.shape[0], mean_ref.shape[0]
        spot = lax.broadcasted_iota(jnp.int32, (columns, tile), 0)
        lane = lax.broadcasted_iota(jnp.int32, (columns, tile), 1)
        chosen = lax.rem(spot, snaps) == lane
        summed = jnp.zeros((fields, snaps), jnp.float32)

        def table(m):
            row = totals_ref[m, 0:1, :] / totals_ref[m, 2:3, :]
            column = jnp.broadcast_to(row, (tile, columns)).T
            spread = jnp.where(chosen, column, 0.0).reshape(columns // snaps, snaps, tile)
            return jnp.sum(spread, axis=1)[:, 0:snaps]

        mine = table(lax.axis_index("mem"))
        for n in range(members):
            mean_ref[n] = mine[n * fields:(n + 1) * fields]
        for m in range(mems):
            all_of = table(m)
            for n in range(members):
                summed = summed + all_of[n * fields:(n + 1) * fields]
        ensemble_ref[...] = summed / (mems * members)


def finish(raw, fix, totals, members, fields, snaps):
    targets, columns, tile = raw.shape
    steps = 2
    part = targets // steps
    rows = members * fields
    return pl.pallas_call(
        functools.partial(finish_kernel, fields, snaps),
        grid=(steps,),
        in_specs=[
            pl.BlockSpec((part, columns, tile), lambda i: (i, 0, 0)),
            pl.BlockSpec((columns, tile), lambda i: (0, 0)),
            pl.BlockSpec(totals.shape, lambda i: (0, 0, 0)),
        ],
        out_specs=(
            pl.BlockSpec((rows, snaps, part * tile), lambda i: (0, 0, i)),
            pl.BlockSpec((members, fields, snaps), lambda i: (0, 0, 0)),
            pl.BlockSpec((fields, snaps), lambda i: (0, 0)),
        ),
        out_shape=(
            jax.ShapeDtypeStruct((rows, snaps, targets * tile), jnp.float32),
            jax.ShapeDtypeStruct((members, fields, snaps), jnp.float32),
            jax.ShapeDtypeStruct((fields, snaps), jnp.float32),
        ),
        compiler_params=pltpu.CompilerParams(vmem_limit_bytes=16 << 20),
    )(raw, fix, totals)


def on_device(
    surface_fields, land_mask, source_area, target_area, weight_tiles, tile_of, block_of, live_slots
):
    members, fields, snaps, cells = surface_fields.shape
    targets = tile_of.shape[0]
    target_cells = target_area.shape[0]
    raw, totals, fix = main_call(
        surface_fields.reshape(members * fields, snaps, cells),
        land_mask.reshape(1, cells),
        source_area.reshape(1, cells),
        target_area.reshape(1, target_cells),
        weight_tiles,
        tile_of.T,
        block_of.T,
        live_slots.reshape(1, targets),
    )
    regridded, conserved, ensemble = finish(raw, fix, totals, members, fields, snaps)
    return regridded.reshape(members, fields, snaps, target_cells), conserved, ensemble


def solution(mesh):
    placed = (
        P(("grp", "mem"), "fld", None, "band"),
        P("band"),
        P("band"),
        P("band"),
        P(),
        P("band", None),
        P("band", None),
        P("band"),
    )
    return jax.shard_map(
        on_device,
        mesh=mesh,
        in_specs=placed,
        out_specs=(
            P(("grp", "mem"), "fld", None, "band"),
            P(("grp", "mem"), "fld", None),
            P(("grp", "fld"), None),
        ),
        check_vma=False,
    )
```
